128 devices in a mesh: dev: 128 (over z, y, x, core).
Axes of the slice: x: 4, y: 4, z: 4, core: 2. Of those that a mesh axis runs over, the one named last changes fastest.
Arguments:
- orbitals: bfloat16 [128, 768, 6144], P('dev'), may hold values from -0.21875 to 0.21875
- density_blocks: bfloat16 [512, 16, 128, 128], P('dev'), may hold values from -1.625 to 2.625
- kinetic_blocks: float32 [512, 16, 128, 128], P('dev'), may hold values from -0.6 to 0.6
- hartree: float32 [768, 8, 128], P('dev'), may hold values from -6 to 6
- vectors: bfloat16 [65536, 256], P('dev'), may hold values from -6 to 6
- brick_blocks: int32 [128, 6], replicated, may hold values from 0 to 511, as said below
- neighbours: int32 [512, 16], replicated, may hold values from 0 to 511, as said below
Outputs:
- potential: float32 [768, 8, 128], P('dev')
- hamiltonian: float32 [512, 16, 128, 128], P('dev')
- first_term: bfloat16 [65536, 256], P('dev')
- second_term: bfloat16 [65536, 256], P('dev')
The draws below stay inside these ranges and needn't reach their ends.
Inputs may be any that keep to these rules, and one draw needn't show every extreme that they name: `brick_blocks`: block b is held by device b // 4. Each brick names 6 different blocks, each held by a device at most 2 indices away from the brick's device, counting cyclically; any two blocks of one brick appear in each other's neighbour lists. `neighbours`: each row names 16 different blocks, the row's own block among them, each held by a device at most 3 indices away from the row's device, counting cyclically.
All inputs are finite; a program needn't handle non-finite values.
Results may differ from the reference program's by a relative error of at most 0.0064.
Values may be sent and summed in bfloat16 or wider, within the bound.
A program may use at most 128 MiB of HBM per device.

```python
import math
import jax
import jax.numpy as jnp
from jax import lax

BLOCK = 128
NEIGH = 16
BPD = 4
BRB = 6
GX = 6
GY = 8
GZ = 128
VEC = 256
NB = 512
ORB = 65536
BRICKS = 128
PTS = 6144
OBR = 768


def shuffled(key, rows, length):
    scores = jax.random.randint(key, (rows, length), 0, 1 << 20)
    scores = scores * length + jnp.arange(length, dtype=jnp.int32)[None, :]
    return jnp.argsort(scores, axis=1, stable=True).astype(jnp.int32)


def layout(key):
    windows = NB // 8
    order = shuffled(jax.random.fold_in(key, 11), windows, 8)
    placed = (order + 8 * jnp.arange(windows, dtype=jnp.int32)[:, None]).reshape(-1)
    spot = jnp.zeros((NB,), jnp.int32).at[placed].set(jnp.arange(NB, dtype=jnp.int32))
    return (placed, spot)


def draw_brick_blocks(key, part):
    placed, spot = layout(key)
    start = BPD * jnp.arange(BRICKS, dtype=jnp.int32)[:, None] - 1
    order = shuffled(jax.random.fold_in(key, 12), BRICKS, BRB)
    return placed[(start + order) % NB].astype(jnp.int32)


def draw_neighbours(key, part):
    placed, spot = layout(key)
    moves = jnp.arange(NEIGH, dtype=jnp.int32) - 7
    order = shuffled(jax.random.fold_in(key, 13), NB, NEIGH)
    return placed[(spot[:, None] + moves[order]) % NB].astype(jnp.int32)


def draw_density_blocks(key, part):
    neigh_list = draw_neighbours(key, part)
    own_block = (neigh_list == jnp.arange(NB, dtype=jnp.int32)[:, None]).astype(jnp.float32)
    noise_key = jax.random.fold_in(key, 14)
    noise = 0.4 * jax.random.truncated_normal(noise_key, -4.0, 4.0, (NB, NEIGH, BLOCK, BLOCK), jnp.float32)
    identity = jnp.eye(BLOCK, dtype=jnp.float32)
    return (noise + own_block[:, :, None, None] * identity).astype(jnp.bfloat16)


def steps_of(stream_key, extent, cuts, smallest, high):
    def one(position, blocks):
        heights = jax.random.uniform(jax.random.fold_in(jax.random.fold_in(stream_key, 6), position), (blocks,), jnp.float32, smallest / len(cuts), high / len(cuts))
        return jnp.repeat(jnp.exp(heights), extent[position] // blocks).reshape((-1,) + (1,) * (len(extent) - position - 1))

    level = one(*cuts[0])
    for cut in cuts[1:]:
        level = level * one(*cut)
    return level


def normal_values(key, dims, deviation, bound, split=(), held_as=jnp.bfloat16):
    gain = steps_of(key, dims, split, -0.22, 0.18) if split else 1.0
    drawn = jax.random.normal(key, dims, jnp.float32) * deviation * gain
    return jnp.minimum(jnp.maximum(drawn, -bound), bound).astype(held_as)


def setup_inputs(seed: int = 0) -> dict:
    streams_of = jax.random.split(jax.random.key(seed), 8)
    orbitals = normal_values(streams_of[0], (BRICKS, OBR, PTS), OBR ** -0.5, 0.21875, ((0, 128),))
    density_blocks = draw_density_blocks(jax.random.fold_in(streams_of[7], 71), 0)
    kinetic_blocks = normal_values(streams_of[2], (NB, NEIGH, BLOCK, BLOCK), 0.1, 0.6, ((0, 128),), jnp.float32)
    hartree = normal_values(streams_of[3], (BRICKS * GX, GY, GZ), 1.0, 6.0, ((0, 128),), jnp.float32)
    vectors = normal_values(streams_of[4], (ORB, VEC), 1.0, 6.0, ((0, 128),))
    brick_blocks = draw_brick_blocks(jax.random.fold_in(streams_of[7], 71), 0)
    neighbours = draw_neighbours(jax.random.fold_in(streams_of[7], 71), 0)
    return {"orbitals": orbitals, "density_blocks": density_blocks, "kinetic_blocks": kinetic_blocks, "hartree": hartree, "vectors": vectors, "brick_blocks": brick_blocks, "neighbours": neighbours}


density_floor = 0.1
grid_step = 0.04
volume_step = 0.25
kappa_pbe = 0.804
mu_pbe = 0.2195

def exchange_energy(values, squares):
    slater = 0.75 * (3.0 / math.pi) ** (1.0 / 3.0)
    reduced = squares / (4.0 * (3.0 * math.pi ** 2) ** (2.0 / 3.0) * values ** (8.0 / 3.0))
    factor = 1.0 + kappa_pbe - kappa_pbe / (1.0 + mu_pbe * reduced / kappa_pbe)
    return -slater * values ** (4.0 / 3.0) * factor

def total_energy(values, squares):
    return jnp.sum(exchange_energy(values, squares))

def potential_terms(values, squares):
    return jax.grad(total_energy, argnums=(0, 1))(values, squares)

def central(field, axis):
    return (jnp.roll(field, -1, axis) - jnp.roll(field, 1, axis)) / (2.0 * grid_step)

def positions(neighbours, row_ids, col_ids):
    matches = neighbours[row_ids] == col_ids[..., None]
    steps = jnp.arange(matches.shape[-1], dtype=jnp.int32)
    return lax.optimization_barrier(jnp.sum(jnp.where(matches, steps, 0), axis=-1)).astype(jnp.int32)

def reference(orbitals, density_blocks, kinetic_blocks, hartree, vectors, brick_blocks, neighbours):
    row_ids = jnp.repeat(brick_blocks[:, :, None], BRB, axis=2)
    col_ids = jnp.repeat(brick_blocks[:, None, :], BRB, axis=1)
    places = positions(neighbours, row_ids, col_ids)

    def brick_density(inputs):
        orbital_rows, rows_here, places_here = inputs
        pair_blocks = density_blocks[rows_here, places_here].astype(jnp.float32)
        matrix = pair_blocks.transpose(0, 2, 1, 3).reshape(OBR, OBR)
        orbital_f = orbital_rows.astype(jnp.float32)
        mixed_terms = jnp.dot(matrix, orbital_f, precision=lax.Precision.HIGHEST)
        return lax.optimization_barrier(jnp.sum(orbital_f * mixed_terms, axis=0))
    density = lax.map(brick_density, (orbitals, row_ids, places))
    clipped = jnp.maximum(density.reshape(BRICKS * GX, GY, GZ), density_floor)
    gradients = [central(clipped, axis) for axis in range(3)]
    grad_square = gradients[0] ** 2 + gradients[1] ** 2 + gradients[2] ** 2
    e_dens, e_sigma = potential_terms(clipped, grad_square)
    divergence = sum((central(2.0 * e_sigma * grad, axis) for axis, grad in enumerate(gradients)))
    potential = hartree + e_dens - divergence
    pot_bricks = potential.reshape(BRICKS, PTS)

    def brick_hamiltonian(carried, inputs):
        orbital_rows, pot_row, rows_here, places_here = inputs
        orbital_f = orbital_rows.astype(jnp.float32)
        weighted = lax.optimization_barrier((orbital_f * pot_row[None, :]).astype(jnp.bfloat16)).astype(jnp.float32)
        brick_part = volume_step * jnp.dot(orbital_f, weighted.T, precision=lax.Precision.HIGHEST)
        pair_part = brick_part.reshape(BRB, BLOCK, BRB, BLOCK).transpose(0, 2, 1, 3)
        return (carried.at[rows_here, places_here].add(pair_part), None)
    hamiltonian, _ = lax.scan(brick_hamiltonian, kinetic_blocks, (orbitals, pot_bricks, row_ids, places))
    coarse = lax.optimization_barrier(hamiltonian.astype(jnp.bfloat16))

    def apply_hamiltonian(vector_rows):
        vector_blocks = vector_rows.astype(jnp.float32).reshape(NB, BLOCK, VEC)

        def one_row(inputs):
            coarse_row, neigh_row = inputs
            return jnp.einsum('kmn,knv->mv', coarse_row.astype(jnp.float32), vector_blocks[neigh_row], precision=lax.Precision.HIGHEST)
        return lax.map(one_row, (coarse, neighbours)).reshape(ORB, VEC)
    first_term = apply_hamiltonian(vectors).astype(jnp.bfloat16)
    second_term = (2.0 * apply_hamiltonian(first_term) - vectors.astype(jnp.float32)).astype(jnp.bfloat16)
    return (potential, hamiltonian, first_term, second_term)
```

```python
import functools
import math

import jax
import jax.numpy as jnp
from jax import lax
from jax.experimental import pallas as pl
from jax.experimental.pallas import tpu as pltpu
from jax.sharding import PartitionSpec as P

MESH = pl.DeviceIdType.MESH
VMEM = pltpu.VMEM
SMEM = pltpu.SMEM
F32 = jnp.float32
BF16 = jnp.bfloat16

density_floor = 0.1
grid_step = 0.04
volume_step = 0.25
kappa_pbe = 0.804
mu_pbe = 0.2195

BLOCK = 128
OWN = 4
WIDTH = 6
NEIGH = 16
PLANES = 6
LINES = 8
ROW = 128
PLANE = LINES * ROW
VEC = 256

FLOWS = 5
SLOTS = FLOWS * OWN


def around(me, count):
    core = lax.rem(me, 2)
    step = 1 - 2 * core
    partner = me + step
    near = lax.rem(me - step + count, count)
    up = lax.rem(me + 2, count)
    down = lax.rem(me + count - 2, count)
    return core, partner, near, up, down


def greet(devices):
    barrier = pltpu.get_barrier_semaphore()
    for device in devices:
        pl.semaphore_signal(barrier, inc=1, device_id=(device,), device_id_type=MESH)
    pl.semaphore_wait(barrier, len(devices))


def remote(src, dst, send_sem, recv_sem, device):
    return pltpu.make_async_remote_copy(
        src_ref=src,
        dst_ref=dst,
        send_sem=send_sem,
        recv_sem=recv_sem,
        device_id=(device,),
        device_id_type=MESH,
    )


BACK = (0, 1, 3, 2)


def row_copies(send, recv, send_sems, recv_sems, cap, devices):
    copies = []
    for flow in range(4):
        rows = OWN if flow == 0 else cap
        copies.append(
            remote(
                send.at[pl.ds(flow * OWN, rows)],
                recv.at[pl.ds(BACK[flow] * OWN, rows)],
                send_sems.at[flow],
                recv_sems.at[BACK[flow]],
                devices[flow],
            )
        )
    return copies


def vector_copies(held, send_sems, recv_sems, me, count, far):
    core, partner, near, up, down = around(me, count)
    step = 1 - 2 * core

    def piece(delta):
        return held.at[pl.ds((delta + 3) * OWN, OWN)]

    def copy(src_delta, dst_delta, sem, device):
        return remote(
            piece(src_delta), piece(dst_delta), send_sems.at[sem], recv_sems.at[sem], device
        )

    first = [
        copy(0, -2, 0, up),
        copy(0, 2, 1, down),
        copy(0, -step, 2, partner),
    ]
    second = [
        copy(-2, -2 - step, 3, partner),
        copy(2, 2 - step, 4, partner),
    ]
    third = []
    if far:
        third.append(copy(2 - 4 * core, 3 - 6 * core, 5, near))
    return first, second, third


def central_roll(field, axis, size):
    after = pltpu.roll(field, size - 1, axis)
    before = pltpu.roll(field, 1, axis)
    return (after - before) / (2.0 * grid_step)


def energy_terms(values, squares):
    slater = 0.75 * (3.0 / math.pi) ** (1.0 / 3.0)
    scale = 4.0 * (3.0 * math.pi**2) ** (2.0 / 3.0)
    cube = jnp.exp(jnp.log(values) * (1.0 / 3.0))
    four = cube * values
    reduced = squares / (scale * four * four)
    inner = 1.0 + mu_pbe * reduced / kappa_pbe
    factor = 1.0 + kappa_pbe - kappa_pbe / inner
    slope = mu_pbe / (inner * inner)
    e_dens = -slater * cube * ((4.0 / 3.0) * factor - (8.0 / 3.0) * reduced * slope)
    e_sigma = -slater * slope / (scale * four)
    return e_dens, e_sigma


def brick_kernel(
    cap,
    far,
    count,
    rows_ref,
    places_ref,
    slot_ref,
    item_ref,
    orb_hbm,
    dens_hbm,
    hartree_ref,
    vec_hbm,
    pot_ref,
    terms_hbm,
    held_hbm,
    orb,
    blocks,
    send,
    recv,
    mat,
    dens,
    part,
    part16,
    tsend,
    local_sems,
    send_sems,
    recv_sems,
    halo_send_sems,
    halo_recv_sems,
    term_send_sems,
    term_recv_sems,
    vec_send_sems,
    vec_recv_sems,
):
    me = lax.axis_index("dev")
    core, partner, near, up, down = around(me, count)
    devices = (partner, near, up, down)
    block_load = pltpu.make_async_copy(dens_hbm, blocks, local_sems.at[0])
    block_load.start()
    orb_load = pltpu.make_async_copy(orb_hbm.at[0], orb, local_sems.at[1])
    orb_load.start()
    own_vec = pltpu.make_async_copy(vec_hbm, held_hbm.at[pl.ds(3 * OWN, OWN)], local_sems.at[2])
    own_vec.start()
    block_load.wait()

    def fill(target, flow, slots):
        def body(i, carry):
            slot = flow * OWN + i
            row = rows_ref[slot]
            for p in range(WIDTH):
                target[slot, p] = blocks[row, places_ref[slot * WIDTH + p]]
            return carry

        lax.fori_loop(0, slots, body, 0)

    for flow in (2, 3, 1):
        fill(send, flow, cap)
    fill(send, 0, OWN)
    greet(devices)
    copies = row_copies(send, recv, send_sems, recv_sems, cap, devices)
    for flow in (1, 2, 3, 0):
        copies[flow].start()
    fill(recv, 4, OWN)
    own_vec.wait()
    first, second, third = vector_copies(held_hbm, vec_send_sems, vec_recv_sems, me, count, far)
    for copy in first:
        copy.start()
    for copy in copies:
        copy.wait()
    for j in range(WIDTH):
        slot = slot_ref[j]
        for p in range(WIDTH):
            mat[pl.ds(j * BLOCK, BLOCK), pl.ds(p * BLOCK, BLOCK)] = recv[slot, p]
    orb_load.wait()

    half = PLANE // 2

    def density_plane(q, carry):
        x = q + 2 * (q // 2)
        x = jnp.where(q >= 4, q - 2, x)
        for h in range(2):
            cols = pl.ds(pl.multiple_of(x * PLANE + h * half, half), half)
            here = orb[:, cols]
            mixed = jnp.dot(mat[...], here, preferred_element_type=F32)
            line = jnp.sum(mixed * here.astype(F32), axis=0, keepdims=True)
            for y in range(LINES // 2):
                dens[x + 2, pl.ds(h * (LINES // 2) + y, 1), :] = jnp.maximum(
                    line[:, y * ROW : (y + 1) * ROW], density_floor
                )
        return carry

    lax.fori_loop(0, 4, density_plane, 0)
    below = lax.rem(me + count - 1, count)
    above = lax.rem(me + 1, count)
    halo_down = remote(
        dens.at[pl.ds(2, 2)], dens.at[pl.ds(8, 2)], halo_send_sems.at[0], halo_recv_sems.at[0], below
    )
    halo_up = remote(
        dens.at[pl.ds(6, 2)], dens.at[pl.ds(0, 2)], halo_send_sems.at[1], halo_recv_sems.at[1], above
    )
    halo_down.start()
    halo_up.start()
    lax.fori_loop(4, 6, density_plane, 0)
    for copy in first:
        copy.wait()
    for copy in second + third:
        copy.start()
    halo_down.wait()
    halo_up.wait()

    field = dens[...]
    mid = field[1:9]
    grad_x = (field[2:10] - field[0:8]) / (2.0 * grid_step)
    grad_y = central_roll(mid, 1, LINES)
    grad_z = central_roll(mid, 2, ROW)
    e_dens, e_sigma = energy_terms(mid, grad_x * grad_x + grad_y * grad_y + grad_z * grad_z)
    twice = 2.0 * e_sigma
    flux_x = twice * grad_x
    divergence = (flux_x[2:8] - flux_x[0:6]) / (2.0 * grid_step)
    divergence = divergence + central_roll((twice * grad_y)[1:7], 1, LINES)
    divergence = divergence + central_roll((twice * grad_z)[1:7], 2, ROW)
    pot_ref[...] = hartree_ref[...] + e_dens[1:7] - divergence

    part[...] = jnp.zeros_like(part)

    def part_plane(q, carry):
        cols = pl.ds(pl.multiple_of(q * half, half), half)
        x = q // 2
        first_line = (q - 2 * x) * (LINES // 2)
        lines = [pot_ref[x, pl.ds(first_line + y, 1), :] for y in range(LINES // 2)]
        scale = jnp.concatenate(lines, axis=1)
        for b in range(3):
            weighted = (orb[pl.ds(256 * b, 256), cols].astype(F32) * scale).astype(BF16)
            top = pl.ds(0, 256 * (b + 1))
            part[top, pl.ds(256 * b, 256)] += lax.dot_general(
                orb[top, cols], weighted, (((1,), (1,)), ((), ())), preferred_element_type=F32
            )
        return carry

    lax.fori_loop(0, 2 * PLANES, part_plane, 0)
    for j in range(WIDTH):
        for p in range(WIDTH):
            if j // 2 <= p // 2:
                tile = part[pl.ds(j * BLOCK, BLOCK), pl.ds(p * BLOCK, BLOCK)]
            else:
                tile = part[pl.ds(p * BLOCK, BLOCK), pl.ds(j * BLOCK, BLOCK)].T
            part16[j, p] = (volume_step * tile).astype(BF16)

    def pick(flow, slots):
        def body(i, carry):
            slot = flow * OWN + i
            tsend[slot] = part16[item_ref[slot]]
            return carry

        lax.fori_loop(0, slots, body, 0)

    term_copies = row_copies(tsend, terms_hbm, term_send_sems, term_recv_sems, cap, devices)
    for flow in (1, 2, 3):
        pick(flow, cap)
        term_copies[flow].start()
    pick(0, OWN)
    term_copies[0].start()
    pick(4, OWN)
    own_terms = pltpu.make_async_copy(
        tsend.at[pl.ds(4 * OWN, OWN)], terms_hbm.at[pl.ds(4 * OWN, OWN)], local_sems.at[3]
    )
    own_terms.start()
    for copy in second + third:
        copy.wait()
    own_terms.wait()
    for copy in term_copies:
        copy.wait()


def brick_stage(cap, far, ident, count, tables, orbitals, density_blocks, hartree, vectors):
    rows, places, slots, items = tables[:4]
    any_spec = pl.BlockSpec(memory_space=pl.ANY)
    vmem_spec = pl.BlockSpec(memory_space=VMEM)
    smem_spec = pl.BlockSpec(memory_space=SMEM)
    pair = (WIDTH, BLOCK, BLOCK)
    dma = pltpu.SemaphoreType.DMA
    return pl.pallas_call(
        functools.partial(brick_kernel, cap, far, count),
        out_shape=(
            jax.ShapeDtypeStruct(hartree.shape, F32),
            jax.ShapeDtypeStruct((SLOTS,) + pair, BF16),
            jax.ShapeDtypeStruct((7 * OWN, BLOCK, VEC), BF16),
        ),
        in_specs=[smem_spec] * 4 + [any_spec, any_spec, vmem_spec, any_spec],
        out_specs=(vmem_spec, any_spec, any_spec),
        scratch_shapes=[
            VMEM(orbitals.shape[1:], BF16),
            VMEM(density_blocks.shape, BF16),
            VMEM((4 * OWN,) + pair, BF16),
            VMEM((SLOTS,) + pair, BF16),
            VMEM((WIDTH * BLOCK, WIDTH * BLOCK), BF16),
            VMEM((PLANES + 4, LINES, ROW), F32),
            VMEM((WIDTH * BLOCK, WIDTH * BLOCK), F32),
            VMEM((WIDTH,) + pair, BF16),
            VMEM((SLOTS,) + pair, BF16),
            dma((4,)),
            dma((4,)),
            dma((4,)),
            dma((2,)),
            dma((2,)),
            dma((4,)),
            dma((4,)),
            dma((6,)),
            dma((6,)),
        ],
        compiler_params=pltpu.CompilerParams(
            collective_id=ident, has_side_effects=True, vmem_limit_bytes=60 * 1024 * 1024
        ),
        name=f"bricks_{cap}",
    )(rows, places, slots, items, orbitals, density_blocks, hartree, vectors)


def first_kernel(
    rows_ref,
    places_ref,
    valid_ref,
    lookup_ref,
    kinetic_ref,
    held_ref,
    terms_hbm,
    ham_ref,
    coarse_ref,
    first_ref,
    terms,
    gathered,
    sems,
):
    s = pl.program_id(0)

    def each(action):
        def body(slot, carry):
            @pl.when(valid_ref[slot] == 1)
            def _():
                action(slot)

            return carry

        lax.fori_loop(0, SLOTS, body, 0)

    def load(slot):
        return pltpu.make_async_copy(terms_hbm.at[slot], terms.at[slot], sems.at[slot])

    @pl.when(s == 0)
    def _():
        each(lambda slot: load(slot).start())

    ham_ref[...] = kinetic_ref[...]

    @pl.when(s == 0)
    def _():
        each(lambda slot: load(slot).wait())

    def add(slot):
        @pl.when(rows_ref[slot] == s)
        def _():
            for p in range(WIDTH):
                k = places_ref[slot * WIDTH + p]
                ham_ref[0, k] = ham_ref[0, k] + terms[slot, p].astype(F32)

    each(add)
    for k in range(NEIGH):
        coarse_ref[0, :, pl.ds(k * BLOCK, BLOCK)] = ham_ref[0, k].astype(BF16)
        gathered[pl.ds(k * BLOCK, BLOCK), :] = held_ref[lookup_ref[s * NEIGH + k]]
    first_ref[0] = jnp.dot(
        coarse_ref[0], gathered[...], preferred_element_type=F32
    ).astype(BF16)


def first_stage(tables, kinetic_blocks, held, terms):
    rows, places, _, _, valid, lookup = tables
    smem_spec = pl.BlockSpec(memory_space=SMEM)
    return pl.pallas_call(
        first_kernel,
        grid=(OWN,),
        out_shape=(
            jax.ShapeDtypeStruct(kinetic_blocks.shape, F32),
            jax.ShapeDtypeStruct((OWN, BLOCK, NEIGH * BLOCK), BF16),
            jax.ShapeDtypeStruct((OWN, BLOCK, VEC), BF16),
        ),
        in_specs=[smem_spec] * 4
        + [
            pl.BlockSpec((1, NEIGH, BLOCK, BLOCK), lambda s: (s, 0, 0, 0)),
            pl.BlockSpec((7 * OWN, BLOCK, VEC), lambda s: (0, 0, 0)),
            pl.BlockSpec(memory_space=pl.ANY),
        ],
        out_specs=(
            pl.BlockSpec((1, NEIGH, BLOCK, BLOCK), lambda s: (s, 0, 0, 0)),
            pl.BlockSpec((1, BLOCK, NEIGH * BLOCK), lambda s: (s, 0, 0)),
            pl.BlockSpec((1, BLOCK, VEC), lambda s: (s, 0, 0)),
        ),
        scratch_shapes=[
            VMEM(terms.shape, BF16),
            VMEM((NEIGH * BLOCK, VEC), BF16),
            pltpu.SemaphoreType.DMA((SLOTS,)),
        ],
        compiler_params=pltpu.CompilerParams(
            dimension_semantics=("arbitrary",), vmem_limit_bytes=40 * 1024 * 1024
        ),
        name="first",
    )(rows, places, valid, lookup, kinetic_blocks, held, terms)


def second_kernel(
    far,
    count,
    lookup_ref,
    first_hbm,
    coarse_hbm,
    vec_ref,
    out_ref,
    held,
    coarse,
    gathered,
    local_sems,
    send_sems,
    recv_sems,
):
    me = lax.axis_index("dev")
    core, partner, near, up, down = around(me, count)
    own = pltpu.make_async_copy(first_hbm, held.at[pl.ds(3 * OWN, OWN)], local_sems.at[0])
    own.start()
    coarse_load = pltpu.make_async_copy(coarse_hbm, coarse, local_sems.at[1])
    coarse_load.start()
    own.wait()
    greet((partner, near, up, down) if far else (partner, up, down))
    first, second, third = vector_copies(held, send_sems, recv_sems, me, count, far)
    for copy in first:
        copy.start()
    first[0].wait_recv()
    second[0].start()
    first[1].wait_recv()
    for copy in [second[1]] + third:
        copy.start()
    first[2].wait_recv()
    coarse_load.wait()
    for copy in second + third:
        copy.wait_recv()

    def row(s, carry):
        for k in range(NEIGH):
            gathered[pl.ds(k * BLOCK, BLOCK), :] = held[lookup_ref[s * NEIGH + k]]
        total = jnp.dot(coarse[s], gathered[...], preferred_element_type=F32)
        out_ref[s] = (2.0 * total - vec_ref[s].astype(F32)).astype(BF16)
        return carry

    lax.fori_loop(0, OWN, row, 0)
    for copy in first + second + third:
        copy.wait_send()


def second_stage(far, ident, count, lookup, first_term, coarse, vectors):
    any_spec = pl.BlockSpec(memory_space=pl.ANY)
    vmem_spec = pl.BlockSpec(memory_space=VMEM)
    dma = pltpu.SemaphoreType.DMA
    return pl.pallas_call(
        functools.partial(second_kernel, far, count),
        out_shape=jax.ShapeDtypeStruct((OWN, BLOCK, VEC), BF16),
        in_specs=[pl.BlockSpec(memory_space=SMEM), any_spec, any_spec, vmem_spec],
        out_specs=vmem_spec,
        scratch_shapes=[
            VMEM((7 * OWN, BLOCK, VEC), BF16),
            VMEM(coarse.shape, BF16),
            VMEM((NEIGH * BLOCK, VEC), BF16),
            dma((2,)),
            dma((6,)),
            dma((6,)),
        ],
        compiler_params=pltpu.CompilerParams(
            collective_id=ident, has_side_effects=True, vmem_limit_bytes=40 * 1024 * 1024
        ),
        name=f"second_{int(far)}",
    )(lookup, first_term, coarse, vectors)


def index_tables(me, count, brick_blocks, neighbours):
    core, partner, near, up, down = around(me, count)
    devices = jnp.stack([partner, near, up, down, me])
    lists = brick_blocks[devices]
    mine = lists[4]
    slots = jnp.arange(OWN, dtype=jnp.int32)
    my_rows = me * OWN + slots
    my_neigh = lax.dynamic_slice_in_dim(neighbours, me * OWN, OWN, 0)
    kinds = jnp.arange(NEIGH, dtype=jnp.int32)
    match = my_neigh[None, :, None, :] == lists[:, None, :, None]
    place = jnp.sum(jnp.where(match, kinds, 0), axis=-1)
    listed = jnp.any(lists[:, None, :] == my_rows[None, :, None], axis=-1)
    before = jnp.where(slots[None, :] < slots[:, None], 1, 0)
    rank = jnp.sum(jnp.where(listed[:, None, :], before[None], 0), axis=-1)
    chosen = listed[:, None, :] & (rank[:, None, :] == slots[None, :, None])
    rows = jnp.sum(jnp.where(chosen, slots, 0), axis=-1)
    valid = jnp.any(chosen, axis=-1).astype(jnp.int32)
    places = jnp.sum(jnp.where(chosen[..., None], place[:, None], 0), axis=2)
    owners = mine // OWN
    flow = jnp.sum(
        jnp.where(owners[:, None] == devices[None, :], jnp.arange(FLOWS, dtype=jnp.int32), 0), -1
    )
    same = (owners[:, None] == owners[None, :]) & (mine[None, :] < mine[:, None])
    slot = flow * OWN + jnp.sum(same.astype(jnp.int32), axis=-1)
    all_slots = jnp.arange(SLOTS, dtype=jnp.int32)
    items = jnp.arange(WIDTH, dtype=jnp.int32)
    item = jnp.sum(jnp.where(slot[None, :] == all_slots[:, None], items, 0), axis=-1)
    delta = (my_neigh // OWN - me + 3 + count) % count
    lookup = delta * OWN + my_neigh % OWN
    tables = (rows, places, slot, item, valid, lookup)
    return tuple(t.reshape(-1).astype(jnp.int32) for t in tables)


def needs(count, brick_blocks, neighbours):
    owners = brick_blocks // OWN
    here = jnp.arange(count, dtype=jnp.int32)[:, None]
    smaller = brick_blocks[:, None, :] < brick_blocks[:, :, None]
    same = owners[:, None, :] == owners[:, :, None]
    rank = jnp.sum((smaller & same).astype(jnp.int32), axis=-1)
    cross = owners // 2 != here // 2
    most = jnp.max(jnp.where(cross, rank + 1, 0))
    chips = count // 2
    homes = jnp.arange(neighbours.shape[0], dtype=jnp.int32)[:, None] // (2 * OWN)
    apart = (neighbours // (2 * OWN) - homes + chips + 1) % chips
    return most, jnp.any(apart > 2)


def per_device(
    orbitals, density_blocks, kinetic_blocks, hartree, vectors, brick_blocks, neighbours
):
    count = lax.axis_size("dev")
    me = lax.axis_index("dev")
    tables = index_tables(me, count, brick_blocks, neighbours)
    most, far = needs(count, brick_blocks, neighbours)
    level = jnp.where(most <= 1, 0, 1)
    level = jnp.where(far, 1, level).astype(jnp.int32)
    vector_blocks = vectors.reshape(OWN, BLOCK, VEC)
    variants = ((1, False, 1), (OWN, True, 2))

    def run(cap, wide, ident):
        def branch():
            return brick_stage(
                cap, wide, ident, count, tables, orbitals, density_blocks, hartree, vector_blocks
            )

        return branch

    potential, terms, held = lax.switch(level, [run(*v) for v in variants])
    hamiltonian, coarse, first_blocks = first_stage(tables, kinetic_blocks, held, terms)

    def finish(wide, ident):
        def branch():
            return second_stage(wide, ident, count, tables[5], first_blocks, coarse, vector_blocks)

        return branch

    second_blocks = lax.switch(level, [finish(v[1], v[2] + 2) for v in variants])
    return (
        potential,
        hamiltonian,
        first_blocks.reshape(vectors.shape),
        second_blocks.reshape(vectors.shape),
    )


def solution(mesh):
    in_specs = (
        P("dev", None, None),
        P("dev", None, None, None),
        P("dev", None, None, None),
        P("dev", None, None),
        P("dev", None),
        P(),
        P(),
    )
    out_specs = (P("dev", None, None), P("dev", None, None, None), P("dev", None), P("dev", None))
    return jax.shard_map(
        per_device, mesh=mesh, in_specs=in_specs, out_specs=out_specs, check_vma=False
    )
```

```python
import functools
import math

import jax
import jax.numpy as jnp
from jax import lax
from jax.experimental import pallas as pl
from jax.experimental.pallas import tpu as pltpu
from jax.sharding import PartitionSpec as P

MESH = pl.DeviceIdType.MESH
VMEM = pltpu.VMEM
SMEM = pltpu.SMEM
F32 = jnp.float32
BF16 = jnp.bfloat16

density_floor = 0.1
grid_step = 0.04
volume_step = 0.25
kappa_pbe = 0.804
mu_pbe = 0.2195

BLOCK = 128
OWN = 4
WIDTH = 6
NEIGH = 16
PLANES = 6
LINES = 8
ROW = 128
PLANE = LINES * ROW
VEC = 256
STEP = 2
SECOND_LIMIT = 8_000_000
PREP_LIMIT = 60_900_000

FLOWS = 5
SLOTS = FLOWS * OWN
BACK = (0, 1, 3, 2)

T_ROW = 0
T_VALID = T_ROW + SLOTS + 1
T_PLACE = T_VALID + SLOTS + 1
T_SLOT = T_PLACE + (SLOTS + 1) * WIDTH
T_PERM = T_SLOT + WIDTH
T_POS = T_PERM + WIDTH
T_ITEM = T_POS + WIDTH
T_LOOK = T_ITEM + SLOTS
T_SIZE = T_LOOK + OWN * NEIGH
SPAN = 9 * OWN


def around(me, count):
    core = lax.rem(me, 2)
    step = 1 - 2 * core
    partner = me + step
    near = lax.rem(me - step + count, count)
    ahead = lax.rem(me + 2 * step + count, count)
    behind = lax.rem(me - 2 * step + count, count)
    return step, partner, near, ahead, behind


def greet(devices):
    barrier = pltpu.get_barrier_semaphore()
    for device in devices:
        pl.semaphore_signal(barrier, inc=1, device_id=(device,), device_id_type=MESH)


def await_greetings(number):
    pl.semaphore_wait(pltpu.get_barrier_semaphore(), number)


def remote(src, dst, send_sem, recv_sem, device):
    return pltpu.make_async_remote_copy(
        src_ref=src,
        dst_ref=dst,
        send_sem=send_sem,
        recv_sem=recv_sem,
        device_id=(device,),
        device_id_type=MESH,
    )


def row_copies(send, place, send_sems, recv_sems, caps, devices):
    sends, receives = {}, {}
    for flow in range(4):
        back = BACK[flow]
        if caps[flow]:
            slots = pl.ds(flow * OWN, caps[flow])
            there = place(back, caps[flow])
            sends[flow] = remote(
                send.at[slots], there, send_sems.at[flow], recv_sems.at[back], devices[flow]
            )
        if caps[back]:
            slots = pl.ds(flow * OWN, caps[back])
            here = place(flow, caps[back])
            receives[flow] = remote(
                send.at[slots], here, send_sems.at[flow], recv_sems.at[flow], devices[flow]
            )
    return sends, receives


def vector_copies(held, send_sems, recv_sems, me, count, far):
    step, partner, near, ahead, behind = around(me, count)
    up = lax.rem(me + 2, count)
    down = lax.rem(me + count - 2, count)

    def piece(delta):
        return held.at[pl.ds((delta + 3) * OWN, OWN)]

    def copy(src_delta, dst_delta, sem, device):
        return remote(
            piece(src_delta), piece(dst_delta), send_sems.at[sem], recv_sems.at[sem], device
        )

    first = [copy(0, -2, 0, up), copy(0, 2, 1, down), copy(0, -step, 2, partner)]
    second = [copy(-2, -2 - step, 3, partner), copy(2, 2 - step, 4, partner)]
    third = []
    if far:
        third.append(copy(2 * step, 3 * step, 5, near))
    return first, second, third


def central_roll(field, axis, size):
    after = pltpu.roll(field, size - 1, axis)
    before = pltpu.roll(field, 1, axis)
    return (after - before) / (2.0 * grid_step)


def energy_terms(values, squares):
    slater = 0.75 * (3.0 / math.pi) ** (1.0 / 3.0)
    scale = 4.0 * (3.0 * math.pi**2) ** (2.0 / 3.0)
    cube = jnp.exp(jnp.log(values) * (1.0 / 3.0))
    four = cube * values
    reduced = squares / (scale * four * four)
    inner = 1.0 + mu_pbe * reduced / kappa_pbe
    factor = 1.0 + kappa_pbe - kappa_pbe / inner
    slope = mu_pbe / (inner * inner)
    e_dens = -slater * cube * ((4.0 / 3.0) * factor - (8.0 / 3.0) * reduced * slope)
    e_sigma = -slater * slope / (scale * four)
    return e_dens, e_sigma


def prep_kernel(
    count, bricks, neigh, brick_rows, neigh_rows, blocks_hbm, hartree_hbm, vec_hbm,
    table, level_ref, blocks, hartree, vec, inverse, sems,
):
    loads = [
        pltpu.make_async_copy(src, dst, sems.at[i])
        for i, (src, dst) in enumerate(
            ((blocks_hbm, blocks), (hartree_hbm, hartree), (vec_hbm, vec))
        )
    ]
    for load in loads:
        load.start()
    me = lax.axis_index("dev")
    _, *others = around(me, count)
    devices = others + [me]
    blocks = count * OWN

    width = brick_rows.shape
    lists = brick_rows[...]
    brick = lax.broadcasted_iota(jnp.int32, width, 1)
    owner = lists // OWN
    rank = jnp.ones(width, jnp.int32)
    for j in range(WIDTH):
        one = jnp.broadcast_to(lists[j : j + 1], width)
        rank += jnp.where((one // OWN == owner) & (one < lists), 1, 0)
    delta = owner - brick
    delta = jnp.where(delta > count // 2, delta - count, delta)
    delta = jnp.where(delta < -(count // 2), delta + count, delta)
    sided = jnp.where(brick % 2 == 0, delta, -delta)
    near_rows = jnp.max(jnp.where(sided < 0, rank, 0))
    far_rows = jnp.max(jnp.where(sided > 1, rank, 0))
    used = neigh_rows[...] // (2 * OWN)
    home = lax.broadcasted_iota(jnp.int32, used.shape, 1) // (2 * OWN)
    apart = jnp.abs(used - home)
    apart = jnp.minimum(apart, count // 2 - apart)
    chips = jnp.max(apart)
    fits = (near_rows <= 1) & (far_rows == 0) & (chips <= 1)
    level_ref[0] = jnp.where(fits, 0, 1).astype(jnp.int32)

    def near_id(block):
        gap = block - (me - 4) * OWN
        gap = jnp.where(gap < 0, gap + blocks, gap)
        return jnp.where(gap >= blocks, gap - blocks, gap)

    for q in range(T_SIZE):
        table[q] = 0
    for s in range(OWN):
        for k in range(NEIGH):
            gap = near_id(neigh[k, me * OWN + s])
            inverse[s * SPAN + gap] = k
            table[T_LOOK + s * NEIGH + k] = gap - OWN
    for f in range(FLOWS):
        listed = [bricks[p, devices[f]] for p in range(WIDTH)]
        gaps = [near_id(b) for b in listed]
        found = 0
        for s in range(OWN):
            hit = listed[0] == me * OWN + s
            for p in range(1, WIDTH):
                hit = hit | (listed[p] == me * OWN + s)
            slot = jnp.where(hit, f * OWN + found, SLOTS)
            table[T_ROW + slot] = s
            table[T_VALID + slot] = 1
            for p in range(WIDTH):
                gap = jnp.where(hit, s * SPAN + gaps[p], 0)
                table[T_PLACE + slot * WIDTH + p] = inverse[gap]
            found = found + jnp.where(hit, 1, 0)

    listed = [bricks[p, me] for p in range(WIDTH)]
    owners = [b // OWN for b in listed]
    local = [jnp.where(o // 2 == me // 2, 1, 0) for o in owners]
    ahead = 0
    behind = sum(local)
    for j in range(WIDTH):
        slot = 0
        for f in range(FLOWS):
            slot = jnp.where(owners[j] == devices[f], f * OWN, slot)
        for i in range(WIDTH):
            if i != j:
                slot = slot + jnp.where((owners[i] == owners[j]) & (listed[i] < listed[j]), 1, 0)
        place = jnp.where(local[j] == 1, ahead, behind)
        ahead = ahead + local[j]
        behind = behind + 1 - local[j]
        table[T_SLOT + place] = slot
        table[T_PERM + place] = j
        table[T_POS + j] = place
        table[T_ITEM + slot] = place
    for load in loads:
        load.wait()


def prep_stage(count, brick_blocks, neighbours, density_blocks, hartree, vectors):
    brick_blocks, neighbours = brick_blocks.T, neighbours.T
    smem_spec = pl.BlockSpec(memory_space=SMEM)
    vmem_spec = pl.BlockSpec(memory_space=VMEM)
    hbm_spec = pl.BlockSpec(memory_space=pltpu.HBM)
    return pl.pallas_call(
        functools.partial(prep_kernel, count),
        out_shape=(
            jax.ShapeDtypeStruct((T_SIZE,), jnp.int32),
            jax.ShapeDtypeStruct((1,), jnp.int32),
            jax.ShapeDtypeStruct(density_blocks.shape, BF16),
            jax.ShapeDtypeStruct(hartree.shape, F32),
            jax.ShapeDtypeStruct(vectors.shape, BF16),
        ),
        in_specs=[smem_spec, smem_spec, vmem_spec, vmem_spec] + [hbm_spec] * 3,
        out_specs=(smem_spec, smem_spec) + (vmem_spec,) * 3,
        scratch_shapes=[SMEM((OWN * SPAN,), jnp.int32), pltpu.SemaphoreType.DMA((3,))],
        compiler_params=pltpu.CompilerParams(vmem_limit_bytes=PREP_LIMIT),
        name="prep",
    )(brick_blocks, neighbours, brick_blocks, neighbours, density_blocks, hartree, vectors)


def brick_kernel(
    caps,
    far,
    split,
    count,
    table,
    orb_hbm,
    blocks,
    kinetic_hbm,
    hartree_ref,
    vec_ref,
    pot_ref,
    terms,
    held,
    kinetic,
    coarse,
    orb,
    send,
    close,
    cross,
    mat,
    inner,
    dens,
    outer_part,
    inner_part,
    part16,
    tsend,
    local_sems,
    send_sems,
    recv_sems,
    halo_send_sems,
    halo_recv_sems,
    term_send_sems,
    term_recv_sems,
    vec_send_sems,
    vec_recv_sems,
):
    me = lax.axis_index("dev")
    step, partner, near, ahead, behind = around(me, count)
    devices = (partner, near, ahead, behind)
    greet(devices)
    orb_load = pltpu.make_async_copy(orb_hbm, orb, local_sems.at[1])
    orb_load.start()
    own_vec = pltpu.make_async_copy(vec_ref, held.at[pl.ds(3 * OWN, OWN)], local_sems.at[2])
    own_vec.start()

    def fill(target, base, flow, slots):
        def body(i, carry):
            slot = flow * OWN + i
            row = table[T_ROW + slot]
            for p in range(WIDTH):
                target[base + i, p] = blocks[row, table[T_PLACE + slot * WIDTH + p]]
            return carry

        lax.fori_loop(0, slots, body, 0)

    def row_place(flow, slots):
        if flow == 0:
            return close.at[pl.ds(0, slots)]
        return cross.at[pl.ds((flow - 1) * OWN, slots)]

    sends, receives = row_copies(send, row_place, send_sems, recv_sems, caps, devices)
    for flow in (1, 2, 3):
        fill(send, flow * OWN, flow, caps[flow])
    await_greetings(4)
    for flow in (1, 2, 3):
        if flow in sends:
            sends[flow].start()
    fill(send, 0, 0, OWN)
    sends[0].start()
    fill(close, OWN, 4, OWN)
    kinetic_load = pltpu.make_async_copy(kinetic_hbm, kinetic, local_sems.at[3])
    kinetic_load.start()

    def assemble(rows, all_here):
        for a in rows:
            slot = table[T_SLOT + a]
            far_slot = jnp.clip(slot - OWN, 0, 3 * OWN - 1)
            is_far = (slot >= OWN) & (slot < 4 * OWN)
            close_slot = jnp.where(slot < OWN, slot, jnp.maximum(slot - 3 * OWN, 0))
            for p in range(WIDTH):
                tile = close[close_slot, p]
                if all_here:
                    tile = jnp.where(is_far, cross[far_slot, p], tile)
                mat[pl.ds(a * BLOCK, BLOCK), pl.ds(p * BLOCK, BLOCK)] = tile

    def await_cross():
        for flow in (1, 2, 3):
            if flow in receives:
                receives[flow].wait_recv()

    own_vec.wait()
    first, second, third = vector_copies(held, vec_send_sems, vec_recv_sems, me, count, far)

    def row_terms(x, begin, end):
        cols = pl.ds(pl.multiple_of(x * PLANE, PLANE), PLANE)
        here = orb[:, :, cols].reshape(WIDTH * BLOCK, PLANE)
        rows = pl.ds(begin * BLOCK, (end - begin) * BLOCK)
        mixed = jnp.dot(mat[rows, :], here, preferred_element_type=F32)
        total = None
        for a in range(begin, end):
            mine = orb[table[T_PERM + a], :, cols].astype(F32)
            term = mixed[(a - begin) * BLOCK : (a - begin + 1) * BLOCK] * mine
            total = term if total is None else total + term
        return jnp.sum(total, axis=0, keepdims=True)

    def store_line(x, line):
        for y in range(LINES):
            dens[x + 2, pl.ds(y, 1), :] = jnp.maximum(
                line[:, y * ROW : (y + 1) * ROW], density_floor
            )

    def plane_of(q):
        return jnp.where(q >= 4, q - 2, q + 2 * (q // 2))

    def inner_body(q, carry):
        inner[q] = row_terms(plane_of(q), 0, 4)
        return carry

    def outer_body(q, carry):
        x = plane_of(q)
        store_line(x, inner[q] + row_terms(x, 4, WIDTH))
        return carry

    receives[0].wait_recv()
    if not split:
        await_cross()
    assemble(range(4), not split)
    orb_load.wait()
    lax.fori_loop(0, 5, inner_body, 0)
    if split:
        await_cross()
    assemble(range(4, WIDTH), True)
    lax.fori_loop(0, 4, outer_body, 0)
    below = lax.rem(me + count - 1, count)
    above = lax.rem(me + 1, count)
    halo_down = remote(
        dens.at[pl.ds(2, 2)], dens.at[pl.ds(8, 2)], halo_send_sems.at[0], halo_recv_sems.at[0], below
    )
    halo_up = remote(
        dens.at[pl.ds(6, 2)], dens.at[pl.ds(0, 2)], halo_send_sems.at[1], halo_recv_sems.at[1], above
    )
    halo_down.start()
    halo_up.start()
    for copy in first:
        copy.start()
    lax.fori_loop(5, 6, inner_body, 0)
    lax.fori_loop(4, 6, outer_body, 0)
    outer_part[...] = jnp.zeros_like(outer_part)
    inner_part[...] = jnp.zeros_like(inner_part)
    halo_down.wait()
    halo_up.wait()

    field = dens[...]
    mid = field[1:9]
    grad_x = (field[2:10] - field[0:8]) / (2.0 * grid_step)
    grad_y = central_roll(mid, 1, LINES)
    grad_z = central_roll(mid, 2, ROW)
    e_dens, e_sigma = energy_terms(mid, grad_x * grad_x + grad_y * grad_y + grad_z * grad_z)
    twice = 2.0 * e_sigma
    flux_x = twice * grad_x
    divergence = (flux_x[2:8] - flux_x[0:6]) / (2.0 * grid_step)
    divergence = divergence + central_roll((twice * grad_y)[1:7], 1, LINES)
    divergence = divergence + central_roll((twice * grad_z)[1:7], 2, ROW)
    pot_ref[...] = hartree_ref[...] + e_dens[1:7] - divergence

    span = STEP * PLANE

    def scale_of(q):
        lines = [
            pot_ref[q * STEP + x, pl.ds(y, 1), :] for x in range(STEP) for y in range(LINES)
        ]
        return jnp.concatenate(lines, axis=1)

    def rows_of(a, cols):
        pair = [orb[table[T_PERM + a], :, cols], orb[table[T_PERM + a + 1], :, cols]]
        return jnp.concatenate(pair, axis=0)

    def product(left, right):
        return lax.dot_general(
            left, right, (((1,), (1,)), ((), ())), preferred_element_type=F32
        )

    def outer_terms(q, carry):
        cols = pl.ds(pl.multiple_of(q * span, span), span)
        weighted = (rows_of(4, cols).astype(F32) * scale_of(q)).astype(BF16)
        every = orb[:, :, cols].reshape(WIDTH * BLOCK, span)
        outer_part[...] += product(every, weighted).reshape(outer_part.shape)
        return carry

    def inner_terms(q, carry):
        cols = pl.ds(pl.multiple_of(q * span, span), span)
        scale = scale_of(q)
        top, low = rows_of(0, cols), rows_of(2, cols)
        inner_part[pl.ds(0, 256), pl.ds(0, 256)] += product(
            top, (top.astype(F32) * scale).astype(BF16)
        )
        weighted = (low.astype(F32) * scale).astype(BF16)
        both = jnp.concatenate([top, low], axis=0)
        inner_part[:, pl.ds(256, 256)] += product(both, weighted)
        return carry

    def rounded(tile):
        return (volume_step * tile).astype(BF16)

    lax.fori_loop(0, PLANES // STEP, outer_terms, 0)
    for a in (4, 5):
        side = pl.ds((a - 4) * BLOCK, BLOCK)
        for b in range(WIDTH):
            tile = outer_part[table[T_PERM + b], :, side]
            part16[a, b] = rounded(tile.T)
            if b < 4:
                part16[b, a] = rounded(tile)

    def pick(flow, slots):
        def body(i, carry):
            slot = flow * OWN + i
            row = table[T_ITEM + slot]
            for p in range(WIDTH):
                tsend[slot, p] = part16[row, table[T_POS + p]]
            return carry

        lax.fori_loop(0, slots, body, 0)

    def term_place(flow, slots):
        return terms.at[pl.ds(flow * OWN, slots)]

    term_caps = [caps[BACK[flow]] for flow in range(4)]
    term_sends, term_receives = row_copies(
        tsend, term_place, term_send_sems, term_recv_sems, term_caps, devices
    )

    def send_cross():
        for flow in (1, 3, 2):
            if flow in term_sends:
                pick(flow, term_caps[flow])
                term_sends[flow].start()

    if split:
        send_cross()
    for copy in first:
        copy.wait()
    for copy in second + third:
        copy.start()
    lax.fori_loop(0, PLANES // STEP, inner_terms, 0)
    for a in range(4):
        for b in range(4):
            if a // 2 <= b // 2:
                tile = inner_part[pl.ds(a * BLOCK, BLOCK), pl.ds(b * BLOCK, BLOCK)]
            else:
                tile = inner_part[pl.ds(b * BLOCK, BLOCK), pl.ds(a * BLOCK, BLOCK)].T
            part16[a, b] = rounded(tile)
    pick(0, OWN)
    term_sends[0].start()
    if not split:
        send_cross()

    def own_terms(i, carry):
        slot = 4 * OWN + i
        row = table[T_ITEM + slot]
        for p in range(WIDTH):
            terms[slot, p] = part16[row, table[T_POS + p]]
        return carry

    lax.fori_loop(0, OWN, own_terms, 0)
    kinetic_load.wait()

    def convert(s, carry):
        for k in range(NEIGH):
            coarse[s, :, pl.ds(k * BLOCK, BLOCK)] = kinetic[s, k].astype(BF16)
        return carry

    lax.fori_loop(0, OWN, convert, 0)
    for flow in sends:
        sends[flow].wait_send()
    for copy in second + third:
        copy.wait()
    for flow in term_receives:
        term_receives[flow].wait_recv()
    for flow in term_sends:
        term_sends[flow].wait_send()


def brick_stage(variant, count, table, orbitals, density_blocks, kinetic_blocks, hartree, vectors):
    caps, far, split, ident = variant
    any_spec = pl.BlockSpec(memory_space=pltpu.HBM)
    vmem_spec = pl.BlockSpec(memory_space=VMEM)
    pair = (WIDTH, BLOCK, BLOCK)
    points = orbitals.shape[2]
    dma = pltpu.SemaphoreType.DMA
    return pl.pallas_call(
        functools.partial(brick_kernel, caps, far, split, count),
        out_shape=(
            jax.ShapeDtypeStruct(hartree.shape, F32),
            jax.ShapeDtypeStruct((SLOTS,) + pair, BF16),
            jax.ShapeDtypeStruct((7 * OWN, BLOCK, VEC), BF16),
            jax.ShapeDtypeStruct(kinetic_blocks.shape, F32),
            jax.ShapeDtypeStruct((OWN, BLOCK, NEIGH * BLOCK), BF16),
        ),
        in_specs=[pl.BlockSpec(memory_space=SMEM)]
        + [any_spec, vmem_spec, any_spec, vmem_spec, vmem_spec],
        out_specs=(vmem_spec,) * 5,
        scratch_shapes=[
            VMEM((WIDTH, BLOCK, points), BF16),
            VMEM((4 * OWN,) + pair, BF16),
            VMEM((2 * OWN,) + pair, BF16),
            VMEM((3 * OWN,) + pair, BF16),
            VMEM((WIDTH * BLOCK, WIDTH * BLOCK), BF16),
            VMEM((PLANES, 1, PLANE), F32),
            VMEM((PLANES + 4, LINES, ROW), F32),
            VMEM((WIDTH, BLOCK, 2 * BLOCK), F32),
            VMEM((4 * BLOCK, 4 * BLOCK), F32),
            VMEM((WIDTH,) + pair, BF16),
            VMEM((4 * OWN,) + pair, BF16),
            dma((4,)),
            dma((4,)),
            dma((4,)),
            dma((2,)),
            dma((2,)),
            dma((4,)),
            dma((4,)),
            dma((6,)),
            dma((6,)),
        ],
        compiler_params=pltpu.CompilerParams(
            collective_id=ident, has_side_effects=True, vmem_limit_bytes=40 * 1024 * 1024
        ),
        name=f"bricks_{ident}",
    )(
        table,
        orbitals.reshape(WIDTH, BLOCK, points),
        density_blocks,
        kinetic_blocks,
        hartree,
        vectors,
    )


def sum_kernel(table, terms, kinetic, rounded, ham, coarse):
    del kinetic, rounded

    def add(slot, carry):
        @pl.when(table[T_VALID + slot] == 1)
        def _():
            s = table[T_ROW + slot]
            for p in range(WIDTH):
                k = table[T_PLACE + slot * WIDTH + p]
                total = ham[s, k] + terms[slot, p].astype(F32)
                ham[s, k] = total
                columns = pl.ds(pl.multiple_of(k * BLOCK, BLOCK), BLOCK)
                coarse[s, :, columns] = total.astype(BF16)

        return carry

    lax.fori_loop(0, SLOTS, add, 0)


def sum_stage(table, terms, kinetic, rounded):
    vmem_spec = pl.BlockSpec(memory_space=VMEM)
    return pl.pallas_call(
        sum_kernel,
        out_shape=(
            jax.ShapeDtypeStruct(kinetic.shape, F32),
            jax.ShapeDtypeStruct(rounded.shape, BF16),
        ),
        in_specs=[pl.BlockSpec(memory_space=SMEM)] + [vmem_spec] * 3,
        out_specs=(vmem_spec,) * 2,
        input_output_aliases={2: 0, 3: 1},
        compiler_params=pltpu.CompilerParams(vmem_limit_bytes=4 * 1024 * 1024),
        name="sum",
    )(table, terms, kinetic, rounded)


def row_product(table, s, coarse, held):
    rows = [held[table[T_LOOK + s * NEIGH + k]] for k in range(NEIGH)]
    return jnp.dot(coarse[s], jnp.concatenate(rows, axis=0), preferred_element_type=F32)


def first_kernel(far, count, table, coarse, vectors, held, send_sems, recv_sems):
    me = lax.axis_index("dev")
    step, partner, near, ahead, behind = around(me, count)
    friends = (partner, near, ahead, behind) if far else (partner, ahead, behind)
    greet(friends)
    first, second, third = vector_copies(held, send_sems, recv_sems, me, count, far)

    def row(s, carry):
        held[3 * OWN + s] = row_product(table, s, coarse, vectors).astype(BF16)
        return carry

    lax.fori_loop(0, OWN, row, 0)
    await_greetings(len(friends))
    for copy in first:
        copy.start()
    first[0].wait_recv()
    second[0].start()
    first[1].wait_recv()
    for copy in [second[1]] + third:
        copy.start()
    first[2].wait_recv()
    for copy in second + third:
        copy.wait_recv()
    for copy in first + second + third:
        copy.wait_send()


def first_stage(far, ident, count, table, coarse, vectors):
    vmem_spec = pl.BlockSpec(memory_space=VMEM)
    dma = pltpu.SemaphoreType.DMA
    return pl.pallas_call(
        functools.partial(first_kernel, far, count),
        out_shape=jax.ShapeDtypeStruct(vectors.shape, BF16),
        in_specs=[pl.BlockSpec(memory_space=SMEM)] + [vmem_spec] * 2,
        out_specs=vmem_spec,
        scratch_shapes=[dma((6,)), dma((6,))],
        compiler_params=pltpu.CompilerParams(
            collective_id=ident, has_side_effects=True, vmem_limit_bytes=8 * 1024 * 1024
        ),
        name=f"first_{ident}",
    )(table, coarse, vectors)


def second_kernel(
    table,
    held,
    coarse,
    vec_ref,
    ham,
    pot_ref,
    out_hbm,
    first_hbm,
    ham_hbm,
    pot_hbm,
    out,
    sems,
):
    copies = [
        pltpu.make_async_copy(pot_ref, pot_hbm, sems.at[OWN]),
        pltpu.make_async_copy(held.at[pl.ds(3 * OWN, OWN)], first_hbm, sems.at[OWN + 1]),
        pltpu.make_async_copy(ham, ham_hbm, sems.at[OWN + 2]),
    ]
    for copy in copies:
        copy.start()

    def store(s):
        return pltpu.make_async_copy(out.at[s], out_hbm.at[s], sems.at[s])

    def row(s, carry):
        total = row_product(table, s, coarse, held)
        out[s] = (2.0 * total - vec_ref[s].astype(F32)).astype(BF16)
        store(s).start()
        return carry

    lax.fori_loop(0, OWN, row, 0)
    for s in range(OWN):
        store(s).wait()
    for copy in copies:
        copy.wait()


def second_stage(table, held, coarse, vectors, ham, potential):
    vmem_spec = pl.BlockSpec(memory_space=VMEM)
    hbm_spec = pl.BlockSpec(memory_space=pltpu.HBM)
    blocks = jax.ShapeDtypeStruct((OWN, BLOCK, VEC), BF16)
    return pl.pallas_call(
        second_kernel,
        out_shape=(
            blocks,
            blocks,
            jax.ShapeDtypeStruct(ham.shape, F32),
            jax.ShapeDtypeStruct(potential.shape, F32),
        ),
        in_specs=[pl.BlockSpec(memory_space=SMEM)] + [vmem_spec] * 5,
        out_specs=(hbm_spec,) * 4,
        scratch_shapes=[
            VMEM(vectors.shape, BF16),
            pltpu.SemaphoreType.DMA((OWN + 3,)),
        ],
        compiler_params=pltpu.CompilerParams(vmem_limit_bytes=SECOND_LIMIT),
        name="second",
    )(table, held, coarse, vectors, ham, potential)


NARROW = ((OWN, 1, 1, 0), False, True, 1)
GENERAL = ((OWN, OWN, OWN, OWN), True, False, 2)
VARIANTS = (NARROW, GENERAL)


def per_device(
    orbitals, density_blocks, kinetic_blocks, hartree, vectors, brick_blocks, neighbours
):
    count = lax.axis_size("dev")
    table, level, density_rows, hartree_here, vector_blocks = prep_stage(
        count,
        brick_blocks,
        neighbours,
        density_blocks,
        hartree,
        vectors.reshape(OWN, BLOCK, VEC),
    )

    def program(variant):
        def branch():
            potential, terms, held, kinetic, rounded = brick_stage(
                variant,
                count,
                table,
                orbitals,
                density_rows,
                kinetic_blocks,
                hartree_here,
                vector_blocks,
            )
            ham, coarse = sum_stage(table, terms, kinetic, rounded)
            held_first = first_stage(variant[1], variant[3] + 2, count, table, coarse, held)
            second_term, first_term, hamiltonian, potential = second_stage(
                table, held_first, coarse, vector_blocks, ham, potential
            )
            return potential, hamiltonian, first_term, second_term

        return branch

    potential, hamiltonian, first_term, second_term = lax.switch(
        level[0], [program(v) for v in VARIANTS]
    )
    return (
        potential,
        hamiltonian,
        first_term.reshape(vectors.shape),
        second_term.reshape(vectors.shape),
    )


def solution(mesh):
    in_specs = (
        P("dev", None, None),
        P("dev", None, None, None),
        P("dev", None, None, None),
        P("dev", None, None),
        P("dev", None),
        P(),
        P(),
    )
    out_specs = (P("dev", None, None), P("dev", None, None, None), P("dev", None), P("dev", None))
    return jax.shard_map(
        per_device, mesh=mesh, in_specs=in_specs, out_specs=out_specs, check_vma=False
    )
```

```python
import functools
import math

import jax
import jax.numpy as jnp
from jax import lax
from jax.experimental import pallas as pl
from jax.experimental.pallas import tpu as pltpu
from jax.sharding import PartitionSpec as P

MESH = pl.DeviceIdType.MESH
VMEM = pltpu.VMEM
SMEM = pltpu.SMEM
F32 = jnp.float32
BF16 = jnp.bfloat16

density_floor = 0.1
grid_step = 0.04
volume_step = 0.25
kappa_pbe = 0.804
mu_pbe = 0.2195

BLOCK = 128
OWN = 4
BITS = 2
WIDTH = 6
NEIGH = 16
PLANES = 6
LINES = 8
ROW = 128
PLANE = LINES * ROW
VEC = 256
STEP = 2
SECOND_LIMIT = 8_000_000
PREP_LIMIT = 60_900_000

FLOWS = 5
HALF = OWN // 2
FLIGHTS = 6
SLOTS = FLOWS * OWN
BACK = (0, 1, 3, 2)

T_ROW = 0
T_VALID = T_ROW + SLOTS + 1
T_PLACE = T_VALID + SLOTS + 1
T_SLOT = T_PLACE + (SLOTS + 1) * WIDTH
T_PERM = T_SLOT + WIDTH
T_POS = T_PERM + WIDTH
T_ITEM = T_POS + WIDTH
T_LOOK = T_ITEM + SLOTS
T_GET = T_LOOK + OWN * NEIGH
T_SPARE = T_GET + FLOWS * OWN * NEIGH
T_SIZE = T_SPARE + 1
CLOSE = 2 * OWN * WIDTH
CROSS = 3 * OWN * WIDTH
SPAN = 9 * OWN


def around(me, count):
    core = lax.rem(me, 2)
    step = 1 - 2 * core
    partner = me + step
    near = lax.rem(me - step + count, count)
    ahead = lax.rem(me + 2 * step + count, count)
    behind = lax.rem(me - 2 * step + count, count)
    return step, partner, near, ahead, behind


def greet(devices):
    barrier = pltpu.get_barrier_semaphore()
    for device in devices:
        pl.semaphore_signal(barrier, inc=1, device_id=(device,), device_id_type=MESH)


def await_greetings(number):
    pl.semaphore_wait(pltpu.get_barrier_semaphore(), number)


def remote(src, dst, send_sem, recv_sem, device):
    return pltpu.make_async_remote_copy(
        src_ref=src,
        dst_ref=dst,
        send_sem=send_sem,
        recv_sem=recv_sem,
        device_id=(device,),
        device_id_type=MESH,
    )


def row_copies(source, place, send_sems, recv_sems, caps, devices):
    sends, receives = {}, {}
    for flow in range(4):
        back = BACK[flow]
        if caps[flow]:
            here, there = source(flow, caps[flow]), place(back, caps[flow])
            sends[flow] = remote(
                here, there, send_sems.at[flow], recv_sems.at[back], devices[flow]
            )
        if caps[back]:
            gone, here = source(flow, caps[back]), place(flow, caps[back])
            receives[flow] = remote(
                gone, here, send_sems.at[flow], recv_sems.at[flow], devices[flow]
            )
    return sends, receives


def vector_copies(held, send_sems, recv_sems, me, count, far, part):
    step, partner, near, ahead, behind = around(me, count)
    up = lax.rem(me + 2, count)
    down = lax.rem(me + count - 2, count)

    def piece(delta):
        return held.at[pl.ds((delta + 3) * OWN + part * HALF, HALF)]

    def copy(src_delta, dst_delta, sem, device):
        sem = part * FLIGHTS + sem
        return remote(
            piece(src_delta), piece(dst_delta), send_sems.at[sem], recv_sems.at[sem], device
        )

    first = [copy(0, -2, 0, up), copy(0, 2, 1, down), copy(0, -step, 2, partner)]
    second = [copy(-2, -2 - step, 3, partner), copy(2, 2 - step, 4, partner)]
    third = []
    if far:
        third.append(copy(2 * step, 3 * step, 5, near))
    return first, second, third


def central_roll(field, axis, size):
    after = pltpu.roll(field, size - 1, axis)
    before = pltpu.roll(field, 1, axis)
    return (after - before) / (2.0 * grid_step)


def energy_terms(values, squares):
    slater = 0.75 * (3.0 / math.pi) ** (1.0 / 3.0)
    scale = 4.0 * (3.0 * math.pi**2) ** (2.0 / 3.0)
    cube = jnp.exp(jnp.log(values) * (1.0 / 3.0))
    four = cube * values
    reduced = squares / (scale * four * four)
    inner = 1.0 + mu_pbe * reduced / kappa_pbe
    factor = 1.0 + kappa_pbe - kappa_pbe / inner
    slope = mu_pbe / (inner * inner)
    e_dens = -slater * cube * ((4.0 / 3.0) * factor - (8.0 / 3.0) * reduced * slope)
    e_sigma = -slater * slope / (scale * four)
    return e_dens, e_sigma


def prep_kernel(
    count, bricks, neigh, brick_rows, neigh_rows, blocks_hbm, hartree_hbm, vec_hbm,
    table, level_ref, blocks, hartree, vec, inverse, sems,
):
    loads = [
        pltpu.make_async_copy(src, dst, sems.at[i])
        for i, (src, dst) in enumerate(
            [(blocks_hbm.at[s], blocks.at[s]) for s in range(OWN)]
            + [(hartree_hbm, hartree), (vec_hbm, vec)]
        )
    ]
    for load in loads:
        load.start()
    me = lax.axis_index("dev")
    _, *others = around(me, count)
    devices = others + [me]
    blocks = count * OWN

    width = brick_rows.shape
    lists = brick_rows[...]
    brick = lax.broadcasted_iota(jnp.int32, width, 1)
    owner = lists >> BITS
    rank = jnp.ones(width, jnp.int32)
    for j in range(WIDTH):
        one = jnp.broadcast_to(lists[j : j + 1], width)
        rank += jnp.where((one >> BITS == owner) & (one < lists), 1, 0)
    delta = owner - brick
    delta = jnp.where(delta > count // 2, delta - count, delta)
    delta = jnp.where(delta < -(count // 2), delta + count, delta)
    sided = jnp.where((brick & 1) == 0, delta, -delta)
    from_near = jnp.sum(jnp.where(sided < 0, 1, 0), axis=0, keepdims=True)
    near_rows = jnp.max(from_near)
    far_rows = jnp.max(jnp.where(sided > 1, rank, 0))
    used = neigh_rows[...] >> (BITS + 1)
    home = lax.broadcasted_iota(jnp.int32, used.shape, 1) >> (BITS + 1)
    apart = jnp.abs(used - home)
    apart = jnp.minimum(apart, count // 2 - apart)
    chips = jnp.max(apart)
    fits = (near_rows <= 1) & (far_rows == 0) & (chips <= 1)
    level_ref[0] = jnp.where(fits, 0, 1).astype(jnp.int32)

    def near_id(block):
        gap = block - (me - 4) * OWN
        gap = jnp.where(gap < 0, gap + blocks, gap)
        return jnp.where(gap >= blocks, gap - blocks, gap)

    for q in (*range(T_SLOT), *range(T_ITEM, T_LOOK)):
        table[q] = 0
    for f in range(FLOWS):
        for q in range(OWN * NEIGH):
            table[T_GET + f * OWN * NEIGH + q] = CLOSE if f in (0, 4) else CROSS
    for s in range(OWN):
        for k in range(NEIGH):
            gap = near_id(neigh[k, me * OWN + s])
            inverse[s * SPAN + gap] = k
            table[T_LOOK + s * NEIGH + k] = gap - OWN
    for f in range(FLOWS):
        listed = [bricks[p, devices[f]] for p in range(WIDTH)]
        gaps = [near_id(b) for b in listed]
        found = 0
        for s in range(OWN):
            hit = listed[0] == me * OWN + s
            for p in range(1, WIDTH):
                hit = hit | (listed[p] == me * OWN + s)
            slot = jnp.where(hit, f * OWN + found, SLOTS)
            table[T_ROW + slot] = s
            table[T_VALID + slot] = 1
            for p in range(WIDTH):
                k = inverse[jnp.where(hit, s * SPAN + gaps[p], 0)]
                table[T_PLACE + slot * WIDTH + p] = k
                first_slot = {0: 0, 4: OWN}.get(f, (f - 1) * OWN)
                spot = T_GET + (f * OWN + s) * NEIGH + k
                table[jnp.where(hit, spot, T_SPARE)] = (first_slot + found) * WIDTH + p
            found = found + jnp.where(hit, 1, 0)

    listed = [bricks[p, me] for p in range(WIDTH)]
    owners = [b >> BITS for b in listed]
    local = [jnp.where(o >> 1 == me >> 1, 1, 0) for o in owners]
    ahead = 0
    behind = sum(local)
    for j in range(WIDTH):
        slot = 0
        for f in range(FLOWS):
            slot = jnp.where(owners[j] == devices[f], f * OWN, slot)
        for i in range(WIDTH):
            if i != j:
                slot = slot + jnp.where((owners[i] == owners[j]) & (listed[i] < listed[j]), 1, 0)
        place = jnp.where(local[j] == 1, ahead, behind)
        ahead = ahead + local[j]
        behind = behind + 1 - local[j]
        table[T_SLOT + place] = slot
        table[T_PERM + place] = j
        table[T_POS + j] = place
        table[T_ITEM + slot] = place
    for load in loads:
        load.wait()


def prep_stage(count, brick_blocks, neighbours, density_blocks, hartree, vectors):
    brick_blocks, neighbours = brick_blocks.T, neighbours.T
    smem_spec = pl.BlockSpec(memory_space=SMEM)
    vmem_spec = pl.BlockSpec(memory_space=VMEM)
    hbm_spec = pl.BlockSpec(memory_space=pltpu.HBM)
    return pl.pallas_call(
        functools.partial(prep_kernel, count),
        out_shape=(
            jax.ShapeDtypeStruct((T_SIZE,), jnp.int32),
            jax.ShapeDtypeStruct((1,), jnp.int32),
            jax.ShapeDtypeStruct(density_blocks.shape, BF16),
            jax.ShapeDtypeStruct(hartree.shape, F32),
            jax.ShapeDtypeStruct(vectors.shape, BF16),
        ),
        in_specs=[smem_spec, smem_spec, vmem_spec, vmem_spec] + [hbm_spec] * 3,
        out_specs=(smem_spec, smem_spec) + (vmem_spec,) * 3,
        scratch_shapes=[SMEM((OWN * SPAN,), jnp.int32), pltpu.SemaphoreType.DMA((OWN + 2,))],
        compiler_params=pltpu.CompilerParams(vmem_limit_bytes=PREP_LIMIT),
        name="prep",
    )(brick_blocks, neighbours, brick_blocks, neighbours, density_blocks, hartree, vectors)


def row_product(table, s, coarse, held):
    rows = [held[table[T_LOOK + s * NEIGH + k]] for k in range(NEIGH)]
    return jnp.dot(coarse[s], jnp.concatenate(rows, axis=0), preferred_element_type=F32)


def brick_kernel(
    caps,
    far,
    split,
    count,
    table,
    orb_hbm,
    blocks,
    kinetic_hbm,
    hartree_ref,
    vec_ref,
    pot_ref,
    held_first,
    ham,
    coarse,
    held,
    close_terms,
    cross_terms,
    first_send_sems,
    first_recv_sems,
    orb,
    send,
    close,
    cross,
    mat,
    inner,
    dens,
    outer_part,
    inner_part,
    part16,
    tsend,
    other,
    local_sems,
    side_send_sems,
    side_recv_sems,
    send_sems,
    recv_sems,
    halo_send_sems,
    halo_recv_sems,
    term_send_sems,
    term_recv_sems,
    vec_send_sems,
    vec_recv_sems,
):
    me = lax.axis_index("dev")
    step, partner, near, ahead, behind = around(me, count)
    devices = (partner, near, ahead, behind)
    greet(devices)
    orb_load = pltpu.make_async_copy(orb_hbm, orb, local_sems.at[1])
    orb_load.start()
    own_vec = pltpu.make_async_copy(vec_ref, held.at[pl.ds(3 * OWN, OWN)], local_sems.at[2])
    own_vec.start()

    def fill(target, base, flow, slots):
        def body(i, carry):
            slot = flow * OWN + i
            row = table[T_ROW + slot]
            for p in range(WIDTH):
                target[base + i, p] = blocks[row, table[T_PLACE + slot * WIDTH + p]]
            return carry

        lax.fori_loop(0, slots, body, 0)

    def row_place(flow, slots):
        if flow == 0:
            return close.at[pl.ds(0, slots)]
        return cross.at[pl.ds((flow - 1) * OWN, slots)]

    def row_source(flow, slots):
        return send.at[pl.ds(flow * OWN, slots)]

    sends, receives = row_copies(row_source, row_place, send_sems, recv_sems, caps, devices)
    for flow in (1, 2, 3):
        fill(send, flow * OWN, flow, caps[flow])
    if split:
        fill(send, 2 * OWN, 2, 1)
    fill(send, 0, 0, OWN)
    fill(close, OWN, 4, OWN)
    await_greetings(4)
    swap = remote(
        send.at[pl.ds(2 * OWN, 1)], other, side_send_sems.at[0], side_recv_sems.at[0], partner
    )
    if split:
        swap.start()
        sends[0].start()
        swap.wait()
        mine = table[T_VALID + OWN] == 1
        for p in range(WIDTH):
            send[OWN, p] = jnp.where(mine, send[OWN, p], other[0, p])
        sends[1].start()
    else:
        for flow in (1, 2, 3, 0):
            sends[flow].start()
    kinetic_load = pltpu.make_async_copy(kinetic_hbm, ham, local_sems.at[3])
    kinetic_load.start()

    def assemble(rows, all_here):
        for a in rows:
            slot = table[T_SLOT + a]
            far_slot = 0 if split else jnp.clip(slot - OWN, 0, 3 * OWN - 1)
            is_far = (slot >= OWN) & (slot < 4 * OWN)
            close_slot = jnp.where(slot < OWN, slot, jnp.maximum(slot - 3 * OWN, 0))
            for p in range(WIDTH):
                tile = close[close_slot, p]
                if all_here:
                    tile = jnp.where(is_far, cross[far_slot, p], tile)
                mat[pl.ds(a * BLOCK, BLOCK), pl.ds(p * BLOCK, BLOCK)] = tile

    def await_cross():
        for flow in (1, 2, 3):
            if flow in receives:
                receives[flow].wait_recv()

    own_vec.wait()
    parts = [
        vector_copies(held, vec_send_sems, vec_recv_sems, me, count, far, part)
        for part in range(2)
    ]

    def start_vectors(part):
        for copy in parts[part][0]:
            copy.start()

    def row_terms(x, begin, end):
        cols = pl.ds(pl.multiple_of(x * PLANE, PLANE), PLANE)
        here = orb[:, :, cols].reshape(WIDTH * BLOCK, PLANE)
        rows = pl.ds(begin * BLOCK, (end - begin) * BLOCK)
        mixed = jnp.dot(mat[rows, :], here, preferred_element_type=F32)
        total = None
        for a in range(begin, end):
            mine = orb[table[T_PERM + a], :, cols].astype(F32)
            term = mixed[(a - begin) * BLOCK : (a - begin + 1) * BLOCK] * mine
            total = term if total is None else total + term
        return jnp.sum(total, axis=0, keepdims=True)

    def store_line(x, line):
        for y in range(LINES):
            dens[x + 2, pl.ds(y, 1), :] = jnp.maximum(
                line[:, y * ROW : (y + 1) * ROW], density_floor
            )

    def plane_of(q):
        return jnp.where(q >= 4, q - 2, q + 2 * (q // 2))

    def inner_body(q, carry):
        inner[q] = row_terms(plane_of(q), 0, 4)
        return carry

    def outer_body(q, carry):
        x = plane_of(q)
        store_line(x, inner[q] + row_terms(x, 4, WIDTH))
        return carry

    receives[0].wait_recv()
    if not split:
        await_cross()
    assemble(range(4), not split)
    orb_load.wait()
    lax.fori_loop(0, 5, inner_body, 0)
    if split:
        await_cross()
    assemble(range(4, WIDTH), True)
    start_vectors(0)
    lax.fori_loop(0, 4, outer_body, 0)
    below = lax.rem(me + count - 1, count)
    above = lax.rem(me + 1, count)
    halo_down = remote(
        dens.at[pl.ds(2, 2)], dens.at[pl.ds(8, 2)], halo_send_sems.at[0], halo_recv_sems.at[0], below
    )
    halo_up = remote(
        dens.at[pl.ds(6, 2)], dens.at[pl.ds(0, 2)], halo_send_sems.at[1], halo_recv_sems.at[1], above
    )
    halo_down.start()
    halo_up.start()
    start_vectors(1)
    lax.fori_loop(5, 6, inner_body, 0)
    lax.fori_loop(4, 6, outer_body, 0)
    outer_part[...] = jnp.zeros_like(outer_part)
    inner_part[...] = jnp.zeros_like(inner_part)
    halo_down.wait()
    halo_up.wait()

    field = dens[...]
    mid = field[1:9]
    grad_x = (field[2:10] - field[0:8]) / (2.0 * grid_step)
    grad_y = central_roll(mid, 1, LINES)
    grad_z = central_roll(mid, 2, ROW)
    e_dens, e_sigma = energy_terms(mid, grad_x * grad_x + grad_y * grad_y + grad_z * grad_z)
    twice = 2.0 * e_sigma
    flux_x = twice * grad_x
    divergence = (flux_x[2:8] - flux_x[0:6]) / (2.0 * grid_step)
    divergence = divergence + central_roll((twice * grad_y)[1:7], 1, LINES)
    divergence = divergence + central_roll((twice * grad_z)[1:7], 2, ROW)
    pot_ref[...] = hartree_ref[...] + e_dens[1:7] - divergence

    span = STEP * PLANE

    def scale_of(q):
        lines = [
            pot_ref[q * STEP + x, pl.ds(y, 1), :] for x in range(STEP) for y in range(LINES)
        ]
        return jnp.concatenate(lines, axis=1)

    def rows_of(a, cols):
        pair = [orb[table[T_PERM + a], :, cols], orb[table[T_PERM + a + 1], :, cols]]
        return jnp.concatenate(pair, axis=0)

    def product(left, right):
        return lax.dot_general(
            left, right, (((1,), (1,)), ((), ())), preferred_element_type=F32
        )

    def outer_terms(q, carry):
        cols = pl.ds(pl.multiple_of(q * span, span), span)
        weighted = (rows_of(4, cols).astype(F32) * scale_of(q)).astype(BF16)
        every = orb[:, :, cols].reshape(WIDTH * BLOCK, span)
        outer_part[...] += product(every, weighted).reshape(outer_part.shape)
        return carry

    def inner_terms(q, carry):
        cols = pl.ds(pl.multiple_of(q * span, span), span)
        scale = scale_of(q)
        top, low = rows_of(0, cols), rows_of(2, cols)
        inner_part[pl.ds(0, 256), pl.ds(0, 256)] += product(
            top, (top.astype(F32) * scale).astype(BF16)
        )
        weighted = (low.astype(F32) * scale).astype(BF16)
        both = jnp.concatenate([top, low], axis=0)
        inner_part[:, pl.ds(256, 256)] += product(both, weighted)
        return carry

    def rounded(tile):
        return (volume_step * tile).astype(BF16)

    lax.fori_loop(0, PLANES // STEP, outer_terms, 0)
    for a in (4, 5):
        side = pl.ds((a - 4) * BLOCK, BLOCK)
        for b in range(WIDTH):
            tile = outer_part[table[T_PERM + b], :, side]
            part16[a, b] = rounded(tile.T)
            if b < 4:
                part16[b, a] = rounded(tile)

    def pick(flow, slots, target, base):
        def body(i, carry):
            row = WIDTH - 1 if split and flow in (1, 2, 3) else table[T_ITEM + flow * OWN + i]
            for p in range(WIDTH):
                target[base + i * WIDTH + p] = part16[row, table[T_POS + p]]
            return carry

        lax.fori_loop(0, slots, body, 0)

    def term_source(flow, slots):
        return tsend.at[pl.ds(flow * OWN * WIDTH, slots * WIDTH)]

    def term_place(flow, slots):
        if flow == 0:
            return close_terms.at[pl.ds(0, slots * WIDTH)]
        return cross_terms.at[pl.ds((flow - 1) * OWN * WIDTH, slots * WIDTH)]

    term_caps = [caps[BACK[flow]] for flow in range(4)]
    term_sends, term_receives = row_copies(
        term_source, term_place, term_send_sems, term_recv_sems, term_caps, devices
    )

    def send_cross():
        for flow in (1, 3, 2):
            if flow in term_sends:
                pick(flow, term_caps[flow], tsend, flow * OWN * WIDTH)
                term_sends[flow].start()

    if split:
        send_cross()
    lax.fori_loop(0, PLANES // STEP, inner_terms, 0)
    for a in range(4):
        for b in range(4):
            if a // 2 <= b // 2:
                tile = inner_part[pl.ds(a * BLOCK, BLOCK), pl.ds(b * BLOCK, BLOCK)]
            else:
                tile = inner_part[pl.ds(b * BLOCK, BLOCK), pl.ds(a * BLOCK, BLOCK)].T
            part16[a, b] = rounded(tile)
    pick(0, OWN, tsend, 0)
    term_sends[0].start()
    if not split:
        send_cross()
    for first, second, third in parts:
        for copy in first:
            copy.wait()
        for copy in second + third:
            copy.start()

    pick(4, OWN, close_terms, OWN * WIDTH)
    close_terms[CLOSE] = jnp.zeros((BLOCK, BLOCK), BF16)
    cross_terms[CROSS] = jnp.zeros((BLOCK, BLOCK), BF16)

    def term(source, flow, s, k):
        return source[table[T_GET + (flow * OWN + s) * NEIGH + k]].astype(F32)

    def close_row(s, carry):
        for k in range(NEIGH):
            ham[s, k] = ham[s, k] + term(close_terms, 4, s, k) + term(close_terms, 0, s, k)
        return carry

    def last_row(s, carry):
        for k in range(NEIGH):
            total = ham[s, k]
            for flow in (1, 2) if split else (1, 2, 3):
                total = total + term(cross_terms, flow, s, k)
            ham[s, k] = total
            coarse[s, :, pl.ds(k * BLOCK, BLOCK)] = total.astype(BF16)
        held_first[3 * OWN + s] = row_product(table, s, coarse, held).astype(BF16)
        return carry

    forward = remote(
        cross_terms.at[pl.ds(0, WIDTH)],
        cross_terms.at[pl.ds(OWN * WIDTH, WIDTH)],
        side_send_sems.at[1],
        side_recv_sems.at[1],
        partner,
    )
    kinetic_load.wait()
    term_receives[0].wait_recv()
    lax.fori_loop(0, OWN, close_row, 0)
    if split:
        term_receives[1].wait_recv()
        forward.start()
        forward.wait()
    else:
        for flow in (1, 2, 3):
            term_receives[flow].wait_recv()
    for first, second, third in parts:
        for copy in second + third:
            copy.wait()

    parts = [
        vector_copies(held_first, first_send_sems, first_recv_sems, me, count, far, part)
        for part in range(2)
    ]
    for part in range(2):
        lax.fori_loop(part * HALF, (part + 1) * HALF, last_row, 0)
        start_vectors(part)
    for first, second, third in parts:
        first[0].wait_recv()
        second[0].start()
        first[1].wait_recv()
        for copy in [second[1]] + third:
            copy.start()
    for first, second, third in parts:
        first[2].wait_recv()
        for copy in second + third:
            copy.wait_recv()
        for copy in first + second + third:
            copy.wait_send()
    for flow in sends:
        sends[flow].wait_send()
    for flow in term_sends:
        term_sends[flow].wait_send()


def brick_stage(variant, count, table, orbitals, density_blocks, kinetic_blocks, hartree, vectors):
    caps, far, split, ident = variant
    any_spec = pl.BlockSpec(memory_space=pltpu.HBM)
    vmem_spec = pl.BlockSpec(memory_space=VMEM)
    pair = (WIDTH, BLOCK, BLOCK)
    points = orbitals.shape[2]
    dma = pltpu.SemaphoreType.DMA
    return pl.pallas_call(
        functools.partial(brick_kernel, caps, far, split, count),
        out_shape=(
            jax.ShapeDtypeStruct(hartree.shape, F32),
            jax.ShapeDtypeStruct((7 * OWN, BLOCK, VEC), BF16),
            jax.ShapeDtypeStruct(kinetic_blocks.shape, F32),
            jax.ShapeDtypeStruct((OWN, BLOCK, NEIGH * BLOCK), BF16),
        ),
        in_specs=[pl.BlockSpec(memory_space=SMEM)]
        + [any_spec, vmem_spec, any_spec, vmem_spec, vmem_spec],
        out_specs=(vmem_spec,) * 4,
        scratch_shapes=[
            VMEM((7 * OWN, BLOCK, VEC), BF16),
            VMEM((CLOSE + 1, BLOCK, BLOCK), BF16),
            VMEM((CROSS + 1, BLOCK, BLOCK), BF16),
            dma((2 * FLIGHTS,)),
            dma((2 * FLIGHTS,)),
            VMEM((WIDTH, BLOCK, points), BF16),
            VMEM((4 * OWN,) + pair, BF16),
            VMEM((2 * OWN,) + pair, BF16),
            VMEM((3 * OWN,) + pair, BF16),
            VMEM((WIDTH * BLOCK, WIDTH * BLOCK), BF16),
            VMEM((PLANES, 1, PLANE), F32),
            VMEM((PLANES + 4, LINES, ROW), F32),
            VMEM((WIDTH, BLOCK, 2 * BLOCK), F32),
            VMEM((4 * BLOCK, 4 * BLOCK), F32),
            VMEM((WIDTH,) + pair, BF16),
            VMEM((4 * OWN * WIDTH, BLOCK, BLOCK), BF16),
            VMEM((1,) + pair, BF16),
            dma((4,)),
            dma((2,)),
            dma((2,)),
            dma((4,)),
            dma((4,)),
            dma((2,)),
            dma((2,)),
            dma((4,)),
            dma((4,)),
            dma((2 * FLIGHTS,)),
            dma((2 * FLIGHTS,)),
        ],
        compiler_params=pltpu.CompilerParams(
            collective_id=ident, has_side_effects=True, vmem_limit_bytes=40 * 1024 * 1024
        ),
        name=f"bricks_{ident}",
    )(
        table,
        orbitals.reshape(WIDTH, BLOCK, points),
        density_blocks,
        kinetic_blocks,
        hartree,
        vectors,
    )


def second_kernel(
    table,
    held,
    coarse,
    vec_ref,
    ham,
    pot_ref,
    out_hbm,
    first_hbm,
    ham_hbm,
    pot_hbm,
    out,
    sems,
):
    copies = [
        pltpu.make_async_copy(pot_ref, pot_hbm, sems.at[OWN]),
        pltpu.make_async_copy(held.at[pl.ds(3 * OWN, OWN)], first_hbm, sems.at[OWN + 1]),
        pltpu.make_async_copy(ham, ham_hbm, sems.at[OWN + 2]),
    ]
    for copy in copies:
        copy.start()

    def store(s):
        return pltpu.make_async_copy(out.at[s], out_hbm.at[s], sems.at[s])

    def row(s, carry):
        total = row_product(table, s, coarse, held)
        out[s] = (2.0 * total - vec_ref[s].astype(F32)).astype(BF16)
        store(s).start()
        return carry

    lax.fori_loop(0, OWN, row, 0)
    for s in range(OWN):
        store(s).wait()
    for copy in copies:
        copy.wait()


def second_stage(table, held, coarse, vectors, ham, potential):
    vmem_spec = pl.BlockSpec(memory_space=VMEM)
    hbm_spec = pl.BlockSpec(memory_space=pltpu.HBM)
    blocks = jax.ShapeDtypeStruct((OWN, BLOCK, VEC), BF16)
    return pl.pallas_call(
        second_kernel,
        out_shape=(
            blocks,
            blocks,
            jax.ShapeDtypeStruct(ham.shape, F32),
            jax.ShapeDtypeStruct(potential.shape, F32),
        ),
        in_specs=[pl.BlockSpec(memory_space=SMEM)] + [vmem_spec] * 5,
        out_specs=(hbm_spec,) * 4,
        scratch_shapes=[
            VMEM(vectors.shape, BF16),
            pltpu.SemaphoreType.DMA((OWN + 3,)),
        ],
        compiler_params=pltpu.CompilerParams(vmem_limit_bytes=SECOND_LIMIT),
        name="second",
    )(table, held, coarse, vectors, ham, potential)


NARROW = ((OWN, 1, 0, 0), False, True, 1)
GENERAL = ((OWN, OWN, OWN, OWN), True, False, 2)
VARIANTS = (NARROW, GENERAL)


def per_device(
    orbitals, density_blocks, kinetic_blocks, hartree, vectors, brick_blocks, neighbours
):
    count = lax.axis_size("dev")
    table, level, density_rows, hartree_here, vector_blocks = prep_stage(
        count,
        brick_blocks,
        neighbours,
        density_blocks,
        hartree,
        vectors.reshape(OWN, BLOCK, VEC),
    )

    def program(variant):
        def branch():
            potential, held_first, ham, coarse = brick_stage(
                variant,
                count,
                table,
                orbitals,
                density_rows,
                kinetic_blocks,
                hartree_here,
                vector_blocks,
            )
            second_term, first_term, hamiltonian, potential = second_stage(
                table, held_first, coarse, vector_blocks, ham, potential
            )
            return potential, hamiltonian, first_term, second_term

        return branch

    potential, hamiltonian, first_term, second_term = lax.switch(
        level[0], [program(v) for v in VARIANTS]
    )
    return (
        potential,
        hamiltonian,
        first_term.reshape(vectors.shape),
        second_term.reshape(vectors.shape),
    )


def solution(mesh):
    in_specs = (
        P("dev", None, None),
        P("dev", None, None, None),
        P("dev", None, None, None),
        P("dev", None, None),
        P("dev", None),
        P(),
        P(),
    )
    out_specs = (P("dev", None, None), P("dev", None, None, None), P("dev", None), P("dev", None))
    return jax.shard_map(
        per_device, mesh=mesh, in_specs=in_specs, out_specs=out_specs, check_vma=False
    )
```

```python
import functools
import math

import jax
import jax.numpy as jnp
from jax import lax
from jax.experimental import pallas as pl
from jax.experimental.pallas import tpu as pltpu
from jax.sharding import PartitionSpec as P

MESH = pl.DeviceIdType.MESH
VMEM = pltpu.VMEM
SMEM = pltpu.SMEM
F32 = jnp.float32
BF16 = jnp.bfloat16

density_floor = 0.1
grid_step = 0.04
volume_step = 0.25
kappa_pbe = 0.804
mu_pbe = 0.2195

BLOCK = 128
OWN = 4
BITS = 2
WIDTH = 6
NEIGH = 16
PLANES = 6
LINES = 8
ROW = 128
PLANE = LINES * ROW
VEC = 256
STEP = 2
SECOND_LIMIT = 8_000_000
PREP_LIMIT = 60_900_000

FLOWS = 5
HALF = OWN // 2
FLIGHTS = 6
SLOTS = FLOWS * OWN
BACK = (0, 1, 3, 2)

T_ROW = 0
T_VALID = T_ROW + SLOTS + 1
T_PLACE = T_VALID + SLOTS + 1
T_SLOT = T_PLACE + (SLOTS + 1) * WIDTH
T_PERM = T_SLOT + WIDTH
T_POS = T_PERM + WIDTH
T_ITEM = T_POS + WIDTH
T_LOOK = T_ITEM + SLOTS
T_GET = T_LOOK + OWN * NEIGH
T_SPARE = T_GET + FLOWS * OWN * NEIGH
T_SIZE = T_SPARE + 1
CLOSE = 2 * OWN * WIDTH
CROSS = 3 * OWN * WIDTH
SPAN = 9 * OWN


def around(me, count):
    core = lax.rem(me, 2)
    step = 1 - 2 * core
    partner = me + step
    near = lax.rem(me - step + count, count)
    ahead = lax.rem(me + 2 * step + count, count)
    behind = lax.rem(me - 2 * step + count, count)
    return step, partner, near, ahead, behind


def greet(devices):
    barrier = pltpu.get_barrier_semaphore()
    for device in devices:
        pl.semaphore_signal(barrier, inc=1, device_id=(device,), device_id_type=MESH)


def await_greetings(number):
    pl.semaphore_wait(pltpu.get_barrier_semaphore(), number)


def remote(src, dst, send_sem, recv_sem, device):
    return pltpu.make_async_remote_copy(
        src_ref=src,
        dst_ref=dst,
        send_sem=send_sem,
        recv_sem=recv_sem,
        device_id=(device,),
        device_id_type=MESH,
    )


def row_copies(source, place, send_sems, recv_sems, caps, devices):
    sends, receives = {}, {}
    for flow in range(4):
        back = BACK[flow]
        if caps[flow]:
            here, there = source(flow, caps[flow]), place(back, caps[flow])
            sends[flow] = remote(
                here, there, send_sems.at[flow], recv_sems.at[back], devices[flow]
            )
        if caps[back]:
            gone, here = source(flow, caps[back]), place(flow, caps[back])
            receives[flow] = remote(
                gone, here, send_sems.at[flow], recv_sems.at[flow], devices[flow]
            )
    return sends, receives


def vector_copies(held, send_sems, recv_sems, me, count, far, part):
    step, partner, near, ahead, behind = around(me, count)
    up = lax.rem(me + 2, count)
    down = lax.rem(me + count - 2, count)

    def piece(delta):
        return held.at[pl.ds((delta + 3) * OWN + part * HALF, HALF)]

    def copy(src_delta, dst_delta, sem, device):
        sem = part * FLIGHTS + sem
        return remote(
            piece(src_delta), piece(dst_delta), send_sems.at[sem], recv_sems.at[sem], device
        )

    first = [copy(0, -2, 0, up), copy(0, 2, 1, down), copy(0, -step, 2, partner)]
    second = [copy(-2, -2 - step, 3, partner), copy(2, 2 - step, 4, partner)]
    third = []
    if far:
        third.append(copy(2 * step, 3 * step, 5, near))
    return first, second, third


def central_roll(field, axis, size):
    after = pltpu.roll(field, size - 1, axis)
    before = pltpu.roll(field, 1, axis)
    return (after - before) / (2.0 * grid_step)


def energy_terms(values, squares):
    slater = 0.75 * (3.0 / math.pi) ** (1.0 / 3.0)
    scale = 4.0 * (3.0 * math.pi**2) ** (2.0 / 3.0)
    cube = jnp.exp(jnp.log(values) * (1.0 / 3.0))
    four = cube * values
    reduced = squares / (scale * four * four)
    inner = 1.0 + mu_pbe * reduced / kappa_pbe
    factor = 1.0 + kappa_pbe - kappa_pbe / inner
    slope = mu_pbe / (inner * inner)
    e_dens = -slater * cube * ((4.0 / 3.0) * factor - (8.0 / 3.0) * reduced * slope)
    e_sigma = -slater * slope / (scale * four)
    return e_dens, e_sigma


def prep_kernel(
    count, bricks, neigh, brick_rows, neigh_rows, blocks_hbm, hartree_hbm, vec_hbm,
    table, level_ref, blocks, hartree, vec, inverse, sems,
):
    loads = [
        pltpu.make_async_copy(src, dst, sems.at[i])
        for i, (src, dst) in enumerate(
            [(blocks_hbm.at[s], blocks.at[s]) for s in range(OWN)]
            + [(hartree_hbm, hartree), (vec_hbm, vec)]
        )
    ]
    for load in loads:
        load.start()
    me = lax.axis_index("dev")
    _, *others = around(me, count)
    devices = others + [me]
    blocks = count * OWN

    width = brick_rows.shape
    lists = brick_rows[...]
    brick = lax.broadcasted_iota(jnp.int32, width, 1)
    owner = lists >> BITS
    rank = jnp.ones(width, jnp.int32)
    for j in range(WIDTH):
        one = jnp.broadcast_to(lists[j : j + 1], width)
        rank += jnp.where((one >> BITS == owner) & (one < lists), 1, 0)
    delta = owner - brick
    delta = jnp.where(delta > count // 2, delta - count, delta)
    delta = jnp.where(delta < -(count // 2), delta + count, delta)
    sided = jnp.where((brick & 1) == 0, delta, -delta)
    from_near = jnp.sum(jnp.where(sided < 0, 1, 0), axis=0, keepdims=True)
    near_rows = jnp.max(from_near)
    far_rows = jnp.max(jnp.where(sided > 1, rank, 0))
    used = neigh_rows[...] >> (BITS + 1)
    home = lax.broadcasted_iota(jnp.int32, used.shape, 1) >> (BITS + 1)
    apart = jnp.abs(used - home)
    apart = jnp.minimum(apart, count // 2 - apart)
    chips = jnp.max(apart)
    fits = (near_rows <= 1) & (far_rows == 0) & (chips <= 1)
    level_ref[0] = jnp.where(fits, 0, 1).astype(jnp.int32)

    def near_id(block):
        gap = block - (me - 4) * OWN
        gap = jnp.where(gap < 0, gap + blocks, gap)
        return jnp.where(gap >= blocks, gap - blocks, gap)

    for q in (*range(T_SLOT), *range(T_ITEM, T_LOOK)):
        table[q] = 0
    for f in range(FLOWS):
        for q in range(OWN * NEIGH):
            table[T_GET + f * OWN * NEIGH + q] = CLOSE if f in (0, 4) else CROSS
    for s in range(OWN):
        for k in range(NEIGH):
            gap = near_id(neigh[k, me * OWN + s])
            inverse[s * SPAN + gap] = k
            table[T_LOOK + s * NEIGH + k] = gap - OWN
    for f in range(FLOWS):
        listed = [bricks[p, devices[f]] for p in range(WIDTH)]
        gaps = [near_id(b) for b in listed]
        found = 0
        for s in range(OWN):
            hit = listed[0] == me * OWN + s
            for p in range(1, WIDTH):
                hit = hit | (listed[p] == me * OWN + s)
            slot = jnp.where(hit, f * OWN + found, SLOTS)
            table[T_ROW + slot] = s
            table[T_VALID + slot] = 1
            for p in range(WIDTH):
                k = inverse[jnp.where(hit, s * SPAN + gaps[p], 0)]
                table[T_PLACE + slot * WIDTH + p] = k
                first_slot = {0: 0, 4: OWN}.get(f, (f - 1) * OWN)
                spot = T_GET + (f * OWN + s) * NEIGH + k
                table[jnp.where(hit, spot, T_SPARE)] = (first_slot + found) * WIDTH + p
            found = found + jnp.where(hit, 1, 0)

    listed = [bricks[p, me] for p in range(WIDTH)]
    owners = [b >> BITS for b in listed]
    local = [jnp.where(o >> 1 == me >> 1, 1, 0) for o in owners]
    ahead = 0
    behind = sum(local)
    for j in range(WIDTH):
        slot = 0
        for f in range(FLOWS):
            slot = jnp.where(owners[j] == devices[f], f * OWN, slot)
        for i in range(WIDTH):
            if i != j:
                slot = slot + jnp.where((owners[i] == owners[j]) & (listed[i] < listed[j]), 1, 0)
        place = jnp.where(local[j] == 1, ahead, behind)
        ahead = ahead + local[j]
        behind = behind + 1 - local[j]
        table[T_SLOT + place] = slot
        table[T_PERM + place] = j
        table[T_POS + j] = place
        table[T_ITEM + slot] = place
    for load in loads:
        load.wait()


def prep_stage(count, brick_blocks, neighbours, density_blocks, hartree, vectors):
    brick_blocks, neighbours = brick_blocks.T, neighbours.T
    smem_spec = pl.BlockSpec(memory_space=SMEM)
    vmem_spec = pl.BlockSpec(memory_space=VMEM)
    hbm_spec = pl.BlockSpec(memory_space=pltpu.HBM)
    return pl.pallas_call(
        functools.partial(prep_kernel, count),
        out_shape=(
            jax.ShapeDtypeStruct((T_SIZE,), jnp.int32),
            jax.ShapeDtypeStruct((1,), jnp.int32),
            jax.ShapeDtypeStruct(density_blocks.shape, BF16),
            jax.ShapeDtypeStruct(hartree.shape, F32),
            jax.ShapeDtypeStruct(vectors.shape, BF16),
        ),
        in_specs=[smem_spec, smem_spec, vmem_spec, vmem_spec] + [hbm_spec] * 3,
        out_specs=(smem_spec, smem_spec) + (vmem_spec,) * 3,
        scratch_shapes=[SMEM((OWN * SPAN,), jnp.int32), pltpu.SemaphoreType.DMA((OWN + 2,))],
        compiler_params=pltpu.CompilerParams(vmem_limit_bytes=PREP_LIMIT),
        name="prep",
    )(brick_blocks, neighbours, brick_blocks, neighbours, density_blocks, hartree, vectors)


def row_product(table, s, coarse, held):
    rows = [held[table[T_LOOK + s * NEIGH + k]] for k in range(NEIGH)]
    return jnp.dot(coarse[s], jnp.concatenate(rows, axis=0), preferred_element_type=F32)


def brick_kernel(
    caps,
    far,
    split,
    count,
    table,
    orb_hbm,
    blocks,
    kinetic_hbm,
    hartree_ref,
    vec_ref,
    pot_ref,
    held_first,
    ham,
    coarse,
    held,
    close_terms,
    cross_terms,
    first_send_sems,
    first_recv_sems,
    orb,
    send,
    close,
    cross,
    mat,
    inner,
    dens,
    outer_part,
    inner_part,
    part16,
    tsend,
    other,
    local_sems,
    side_send_sems,
    side_recv_sems,
    send_sems,
    recv_sems,
    halo_send_sems,
    halo_recv_sems,
    term_send_sems,
    term_recv_sems,
    vec_send_sems,
    vec_recv_sems,
):
    me = lax.axis_index("dev")
    step, partner, near, ahead, behind = around(me, count)
    devices = (partner, near, ahead, behind)
    greet(devices)
    orb_load = pltpu.make_async_copy(orb_hbm, orb, local_sems.at[1])
    orb_load.start()
    own_vec = pltpu.make_async_copy(vec_ref, held.at[pl.ds(3 * OWN, OWN)], local_sems.at[2])
    own_vec.start()

    def fill(target, base, flow, slots):
        def body(i, carry):
            slot = flow * OWN + i
            row = table[T_ROW + slot]
            for p in range(WIDTH):
                target[base + i, p] = blocks[row, table[T_PLACE + slot * WIDTH + p]]
            return carry

        lax.fori_loop(0, slots, body, 0)

    def row_place(flow, slots):
        if flow == 0:
            return close.at[pl.ds(0, slots)]
        return cross.at[pl.ds((flow - 1) * OWN, slots)]

    def row_source(flow, slots):
        return send.at[pl.ds(flow * OWN, slots)]

    sends, receives = row_copies(row_source, row_place, send_sems, recv_sems, caps, devices)
    for flow in (1, 2, 3):
        fill(send, flow * OWN, flow, caps[flow])
    if split:
        fill(send, 2 * OWN, 2, 1)
    fill(send, 0, 0, OWN)
    fill(close, OWN, 4, OWN)
    await_greetings(4)
    swap = remote(
        send.at[pl.ds(2 * OWN, 1)], other, side_send_sems.at[0], side_recv_sems.at[0], partner
    )
    if split:
        swap.start()
        sends[0].start()
        swap.wait()
        mine = table[T_VALID + OWN] == 1
        for p in range(WIDTH):
            send[OWN, p] = jnp.where(mine, send[OWN, p], other[0, p])
        sends[1].start()
    else:
        for flow in (1, 2, 3, 0):
            sends[flow].start()
    kinetic_load = pltpu.make_async_copy(kinetic_hbm, ham, local_sems.at[3])
    kinetic_load.start()

    def assemble(rows, all_here):
        for a in rows:
            slot = table[T_SLOT + a]
            far_slot = 0 if split else jnp.clip(slot - OWN, 0, 3 * OWN - 1)
            is_far = (slot >= OWN) & (slot < 4 * OWN)
            close_slot = jnp.where(slot < OWN, slot, jnp.maximum(slot - 3 * OWN, 0))
            for p in range(WIDTH):
                tile = close[close_slot, p]
                if all_here:
                    tile = jnp.where(is_far, cross[far_slot, p], tile)
                mat[pl.ds(a * BLOCK, BLOCK), pl.ds(p * BLOCK, BLOCK)] = tile

    def await_cross():
        for flow in (1, 2, 3):
            if flow in receives:
                receives[flow].wait_recv()

    own_vec.wait()
    parts = [
        vector_copies(held, vec_send_sems, vec_recv_sems, me, count, far, part)
        for part in range(2)
    ]

    def start_vectors(part):
        for copy in parts[part][0]:
            copy.start()

    def row_terms(x, begin, end):
        cols = pl.ds(pl.multiple_of(x * PLANE, PLANE), PLANE)
        here = orb[:, :, cols].reshape(WIDTH * BLOCK, PLANE)
        rows = pl.ds(begin * BLOCK, (end - begin) * BLOCK)
        mixed = jnp.dot(mat[rows, :], here, preferred_element_type=F32)
        total = None
        for a in range(begin, end):
            mine = orb[table[T_PERM + a], :, cols].astype(F32)
            term = mixed[(a - begin) * BLOCK : (a - begin + 1) * BLOCK] * mine
            total = term if total is None else total + term
        return jnp.sum(total, axis=0, keepdims=True)

    def store_line(x, line):
        for y in range(LINES):
            dens[x + 2, pl.ds(y, 1), :] = jnp.maximum(
                line[:, y * ROW : (y + 1) * ROW], density_floor
            )

    def plane_of(q):
        return jnp.where(q >= 4, q - 2, q + 2 * (q // 2))

    def inner_body(q, carry):
        inner[q] = row_terms(plane_of(q), 0, 4)
        return carry

    def outer_body(q, carry):
        x = plane_of(q)
        store_line(x, inner[q] + row_terms(x, 4, WIDTH))
        return carry

    receives[0].wait_recv()
    if not split:
        await_cross()
    assemble(range(4), not split)
    orb_load.wait()
    lax.fori_loop(0, 5, inner_body, 0)
    if split:
        await_cross()
    assemble(range(4, WIDTH), True)
    lax.fori_loop(0, 4, outer_body, 0)
    below = lax.rem(me + count - 1, count)
    above = lax.rem(me + 1, count)
    halo_down = remote(
        dens.at[pl.ds(2, 2)], dens.at[pl.ds(8, 2)], halo_send_sems.at[0], halo_recv_sems.at[0], below
    )
    halo_up = remote(
        dens.at[pl.ds(6, 2)], dens.at[pl.ds(0, 2)], halo_send_sems.at[1], halo_recv_sems.at[1], above
    )
    halo_down.start()
    halo_up.start()
    start_vectors(0)
    start_vectors(1)
    lax.fori_loop(5, 6, inner_body, 0)
    lax.fori_loop(4, 6, outer_body, 0)
    outer_part[...] = jnp.zeros_like(outer_part)
    inner_part[...] = jnp.zeros_like(inner_part)
    halo_down.wait()
    halo_up.wait()

    field = dens[...]
    mid = field[1:9]
    grad_x = (field[2:10] - field[0:8]) / (2.0 * grid_step)
    grad_y = central_roll(mid, 1, LINES)
    grad_z = central_roll(mid, 2, ROW)
    e_dens, e_sigma = energy_terms(mid, grad_x * grad_x + grad_y * grad_y + grad_z * grad_z)
    twice = 2.0 * e_sigma
    flux_x = twice * grad_x
    divergence = (flux_x[2:8] - flux_x[0:6]) / (2.0 * grid_step)
    divergence = divergence + central_roll((twice * grad_y)[1:7], 1, LINES)
    divergence = divergence + central_roll((twice * grad_z)[1:7], 2, ROW)
    pot_ref[...] = hartree_ref[...] + e_dens[1:7] - divergence

    span = STEP * PLANE

    def scale_of(q):
        lines = [
            pot_ref[q * STEP + x, pl.ds(y, 1), :] for x in range(STEP) for y in range(LINES)
        ]
        return jnp.concatenate(lines, axis=1)

    def rows_of(a, cols):
        pair = [orb[table[T_PERM + a], :, cols], orb[table[T_PERM + a + 1], :, cols]]
        return jnp.concatenate(pair, axis=0)

    def product(left, right):
        return lax.dot_general(
            left, right, (((1,), (1,)), ((), ())), preferred_element_type=F32
        )

    def outer_terms(q, carry):
        cols = pl.ds(pl.multiple_of(q * span, span), span)
        weighted = (rows_of(4, cols).astype(F32) * scale_of(q)).astype(BF16)
        every = orb[:, :, cols].reshape(WIDTH * BLOCK, span)
        outer_part[...] += product(every, weighted).reshape(outer_part.shape)
        return carry

    def inner_terms(q, carry):
        cols = pl.ds(pl.multiple_of(q * span, span), span)
        scale = scale_of(q)
        top, low = rows_of(0, cols), rows_of(2, cols)
        inner_part[pl.ds(0, 256), pl.ds(0, 256)] += product(
            top, (top.astype(F32) * scale).astype(BF16)
        )
        weighted = (low.astype(F32) * scale).astype(BF16)
        both = jnp.concatenate([top, low], axis=0)
        inner_part[:, pl.ds(256, 256)] += product(both, weighted)
        return carry

    def rounded(tile):
        return (volume_step * tile).astype(BF16)

    lax.fori_loop(0, PLANES // STEP, outer_terms, 0)
    for a in (4, 5):
        side = pl.ds((a - 4) * BLOCK, BLOCK)
        for b in range(WIDTH):
            tile = outer_part[table[T_PERM + b], :, side]
            part16[a, b] = rounded(tile.T)
            if b < 4:
                part16[b, a] = rounded(tile)

    def pick(flow, slots, target, base):
        def body(i, carry):
            row = WIDTH - 1 if split and flow in (1, 2, 3) else table[T_ITEM + flow * OWN + i]
            for p in range(WIDTH):
                target[base + i * WIDTH + p] = part16[row, table[T_POS + p]]
            return carry

        lax.fori_loop(0, slots, body, 0)

    def term_source(flow, slots):
        return tsend.at[pl.ds(flow * OWN * WIDTH, slots * WIDTH)]

    def term_place(flow, slots):
        if flow == 0:
            return close_terms.at[pl.ds(0, slots * WIDTH)]
        return cross_terms.at[pl.ds((flow - 1) * OWN * WIDTH, slots * WIDTH)]

    term_caps = [caps[BACK[flow]] for flow in range(4)]
    term_sends, term_receives = row_copies(
        term_source, term_place, term_send_sems, term_recv_sems, term_caps, devices
    )

    def send_cross():
        for flow in (1, 3, 2):
            if flow in term_sends:
                pick(flow, term_caps[flow], tsend, flow * OWN * WIDTH)
                term_sends[flow].start()

    if split:
        send_cross()
    lax.fori_loop(0, PLANES // STEP, inner_terms, 0)
    for a in range(4):
        for b in range(4):
            if a // 2 <= b // 2:
                tile = inner_part[pl.ds(a * BLOCK, BLOCK), pl.ds(b * BLOCK, BLOCK)]
            else:
                tile = inner_part[pl.ds(b * BLOCK, BLOCK), pl.ds(a * BLOCK, BLOCK)].T
            part16[a, b] = rounded(tile)
    pick(0, OWN, tsend, 0)
    term_sends[0].start()
    if not split:
        send_cross()
    for first, second, third in parts:
        for copy in first:
            copy.wait()
        for copy in second + third:
            copy.start()

    pick(4, OWN, close_terms, OWN * WIDTH)
    close_terms[CLOSE] = jnp.zeros((BLOCK, BLOCK), BF16)
    cross_terms[CROSS] = jnp.zeros((BLOCK, BLOCK), BF16)

    def term(source, flow, s, k):
        return source[table[T_GET + (flow * OWN + s) * NEIGH + k]].astype(F32)

    def close_row(s, carry):
        for k in range(NEIGH):
            ham[s, k] = ham[s, k] + term(close_terms, 4, s, k) + term(close_terms, 0, s, k)
        return carry

    def last_row(s, carry):
        for k in range(NEIGH):
            total = ham[s, k]
            for flow in (1, 2) if split else (1, 2, 3):
                total = total + term(cross_terms, flow, s, k)
            ham[s, k] = total
            coarse[s, :, pl.ds(k * BLOCK, BLOCK)] = total.astype(BF16)
        held_first[3 * OWN + s] = row_product(table, s, coarse, held).astype(BF16)
        return carry

    forward = remote(
        cross_terms.at[pl.ds(0, WIDTH)],
        cross_terms.at[pl.ds(OWN * WIDTH, WIDTH)],
        side_send_sems.at[1],
        side_recv_sems.at[1],
        partner,
    )
    kinetic_load.wait()
    term_receives[0].wait_recv()
    lax.fori_loop(0, OWN, close_row, 0)
    if split:
        term_receives[1].wait_recv()
        forward.start()
        forward.wait()
    else:
        for flow in (1, 2, 3):
            term_receives[flow].wait_recv()
    for first, second, third in parts:
        for copy in second + third:
            copy.wait()

    parts = [
        vector_copies(held_first, first_send_sems, first_recv_sems, me, count, far, part)
        for part in range(2)
    ]
    for part in range(2):
        lax.fori_loop(part * HALF, (part + 1) * HALF, last_row, 0)
        start_vectors(part)
    for first, second, third in parts:
        first[0].wait_recv()
        second[0].start()
        first[1].wait_recv()
        for copy in [second[1]] + third:
            copy.start()
    for first, second, third in parts:
        first[2].wait_recv()
        for copy in second + third:
            copy.wait_recv()
        for copy in first + second + third:
            copy.wait_send()
    for flow in sends:
        sends[flow].wait_send()
    for flow in term_sends:
        term_sends[flow].wait_send()


def brick_stage(variant, count, table, orbitals, density_blocks, kinetic_blocks, hartree, vectors):
    caps, far, split, ident = variant
    any_spec = pl.BlockSpec(memory_space=pltpu.HBM)
    vmem_spec = pl.BlockSpec(memory_space=VMEM)
    pair = (WIDTH, BLOCK, BLOCK)
    points = orbitals.shape[2]
    dma = pltpu.SemaphoreType.DMA
    return pl.pallas_call(
        functools.partial(brick_kernel, caps, far, split, count),
        out_shape=(
            jax.ShapeDtypeStruct(hartree.shape, F32),
            jax.ShapeDtypeStruct((7 * OWN, BLOCK, VEC), BF16),
            jax.ShapeDtypeStruct(kinetic_blocks.shape, F32),
            jax.ShapeDtypeStruct((OWN, BLOCK, NEIGH * BLOCK), BF16),
        ),
        in_specs=[pl.BlockSpec(memory_space=SMEM)]
        + [any_spec, vmem_spec, any_spec, vmem_spec, vmem_spec],
        out_specs=(vmem_spec,) * 4,
        scratch_shapes=[
            VMEM((7 * OWN, BLOCK, VEC), BF16),
            VMEM((CLOSE + 1, BLOCK, BLOCK), BF16),
            VMEM((CROSS + 1, BLOCK, BLOCK), BF16),
            dma((2 * FLIGHTS,)),
            dma((2 * FLIGHTS,)),
            VMEM((WIDTH, BLOCK, points), BF16),
            VMEM((4 * OWN,) + pair, BF16),
            VMEM((2 * OWN,) + pair, BF16),
            VMEM((3 * OWN,) + pair, BF16),
            VMEM((WIDTH * BLOCK, WIDTH * BLOCK), BF16),
            VMEM((PLANES, 1, PLANE), F32),
            VMEM((PLANES + 4, LINES, ROW), F32),
            VMEM((WIDTH, BLOCK, 2 * BLOCK), F32),
            VMEM((4 * BLOCK, 4 * BLOCK), F32),
            VMEM((WIDTH,) + pair, BF16),
            VMEM((4 * OWN * WIDTH, BLOCK, BLOCK), BF16),
            VMEM((1,) + pair, BF16),
            dma((4,)),
            dma((2,)),
            dma((2,)),
            dma((4,)),
            dma((4,)),
            dma((2,)),
            dma((2,)),
            dma((4,)),
            dma((4,)),
            dma((2 * FLIGHTS,)),
            dma((2 * FLIGHTS,)),
        ],
        compiler_params=pltpu.CompilerParams(
            collective_id=ident, has_side_effects=True, vmem_limit_bytes=40 * 1024 * 1024
        ),
        name=f"bricks_{ident}",
    )(
        table,
        orbitals.reshape(WIDTH, BLOCK, points),
        density_blocks,
        kinetic_blocks,
        hartree,
        vectors,
    )


def second_kernel(
    table,
    held,
    coarse,
    vec_ref,
    ham,
    pot_ref,
    out_hbm,
    first_hbm,
    ham_hbm,
    pot_hbm,
    out,
    sems,
):
    copies = [
        pltpu.make_async_copy(pot_ref, pot_hbm, sems.at[OWN]),
        pltpu.make_async_copy(held.at[pl.ds(3 * OWN, OWN)], first_hbm, sems.at[OWN + 1]),
        pltpu.make_async_copy(ham, ham_hbm, sems.at[OWN + 2]),
    ]
    for copy in copies:
        copy.start()

    def store(s):
        return pltpu.make_async_copy(out.at[s], out_hbm.at[s], sems.at[s])

    def row(s, carry):
        total = row_product(table, s, coarse, held)
        out[s] = (2.0 * total - vec_ref[s].astype(F32)).astype(BF16)
        store(s).start()
        return carry

    lax.fori_loop(0, OWN, row, 0)
    for s in range(OWN):
        store(s).wait()
    for copy in copies:
        copy.wait()


def second_stage(table, held, coarse, vectors, ham, potential):
    vmem_spec = pl.BlockSpec(memory_space=VMEM)
    hbm_spec = pl.BlockSpec(memory_space=pltpu.HBM)
    blocks = jax.ShapeDtypeStruct((OWN, BLOCK, VEC), BF16)
    return pl.pallas_call(
        second_kernel,
        out_shape=(
            blocks,
            blocks,
            jax.ShapeDtypeStruct(ham.shape, F32),
            jax.ShapeDtypeStruct(potential.shape, F32),
        ),
        in_specs=[pl.BlockSpec(memory_space=SMEM)] + [vmem_spec] * 5,
        out_specs=(hbm_spec,) * 4,
        scratch_shapes=[
            VMEM(vectors.shape, BF16),
            pltpu.SemaphoreType.DMA((OWN + 3,)),
        ],
        compiler_params=pltpu.CompilerParams(vmem_limit_bytes=SECOND_LIMIT),
        name="second",
    )(table, held, coarse, vectors, ham, potential)


NARROW = ((OWN, 1, 0, 0), False, True, 1)
GENERAL = ((OWN, OWN, OWN, OWN), True, False, 2)
VARIANTS = (NARROW, GENERAL)


def per_device(
    orbitals, density_blocks, kinetic_blocks, hartree, vectors, brick_blocks, neighbours
):
    count = lax.axis_size("dev")
    table, level, density_rows, hartree_here, vector_blocks = prep_stage(
        count,
        brick_blocks,
        neighbours,
        density_blocks,
        hartree,
        vectors.reshape(OWN, BLOCK, VEC),
    )

    def program(variant):
        def branch():
            potential, held_first, ham, coarse = brick_stage(
                variant,
                count,
                table,
                orbitals,
                density_rows,
                kinetic_blocks,
                hartree_here,
                vector_blocks,
            )
            second_term, first_term, hamiltonian, potential = second_stage(
                table, held_first, coarse, vector_blocks, ham, potential
            )
            return potential, hamiltonian, first_term, second_term

        return branch

    potential, hamiltonian, first_term, second_term = lax.switch(
        level[0], [program(v) for v in VARIANTS]
    )
    return (
        potential,
        hamiltonian,
        first_term.reshape(vectors.shape),
        second_term.reshape(vectors.shape),
    )


def solution(mesh):
    in_specs = (
        P("dev", None, None),
        P("dev", None, None, None),
        P("dev", None, None, None),
        P("dev", None, None),
        P("dev", None),
        P(),
        P(),
    )
    out_specs = (P("dev", None, None), P("dev", None, None, None), P("dev", None), P("dev", None))
    return jax.shard_map(
        per_device, mesh=mesh, in_specs=in_specs, out_specs=out_specs, check_vma=False
    )
```
